8 devices in a mesh: rep: 1 (over z), head: 2 (over y), seq: 4 (over x, core).
Axes of the slice: x: 2, y: 2, z: 1, core: 2. Of those that a mesh axis runs over, the one named last changes fastest.
Arguments:
- tokens: bfloat16 [32, 3072], P('rep')
- w_query: bfloat16 [3072, 4096], replicated
- w_key: bfloat16 [3072, 4096], replicated
- w_value: bfloat16 [3072, 4096], replicated
- w_out: bfloat16 [4096, 3072], P(('head', 'seq'))
- k_cache: bfloat16 [32, 1024, 16, 256], P('rep', 'seq', 'head')
- v_cache: bfloat16 [32, 1024, 16, 256], P('rep', 'seq', 'head')
- positions: int32 [32], P('rep')
Outputs:
- output 1: bfloat16 [32, 3072], P('rep')
- output 2: bfloat16 [32, 1024, 16, 256], P('rep', 'seq', 'head')
- output 3: bfloat16 [32, 1024, 16, 256], P('rep', 'seq', 'head')
All inputs are finite; a program needn't handle non-finite values.
Results may differ from the reference program's by a relative error of at most 0.00595572.
Values are sent between devices in bfloat16 or wider.
A program may use at most 1 GiB of HBM per device.

```python
import math
import jax
import jax.numpy as jnp
from jax import lax

BATCH = 32
D_MODEL = 3072
N_HEADS = 16
N_KV = 16
HEAD_DIM = 256
SHARD_LEN = 256
SEQ_LEN = 1024
KEY_SCALE = math.sqrt(math.log(SHARD_LEN / 16))


def setup_inputs(seed: int = 0, part: int = 0) -> dict:
    base_key = jax.random.key(seed)
    part_key = jax.random.fold_in(base_key, part)
    weight_keys = jax.random.split(base_key, 4)
    part_keys = jax.random.split(part_key, 4)
    tokens = jax.random.normal(part_keys[0], (BATCH, D_MODEL), jnp.float32)
    w_query = jax.random.normal(weight_keys[0], (D_MODEL, N_HEADS * HEAD_DIM), jnp.float32) * D_MODEL ** -0.5
    w_key = jax.random.normal(weight_keys[1], (D_MODEL, N_KV * HEAD_DIM), jnp.float32) * (KEY_SCALE * D_MODEL ** -0.5)
    w_value = jax.random.normal(weight_keys[2], (D_MODEL, N_KV * HEAD_DIM), jnp.float32) * D_MODEL ** -0.5
    w_out = jax.random.normal(weight_keys[3], (N_HEADS * HEAD_DIM, D_MODEL), jnp.float32) * (N_HEADS * HEAD_DIM) ** -0.5
    k_cache = jax.random.normal(part_keys[1], (BATCH, SEQ_LEN, N_KV, HEAD_DIM), jnp.float32) * KEY_SCALE
    v_cache = jax.random.normal(part_keys[2], (BATCH, SEQ_LEN, N_KV, HEAD_DIM), jnp.float32)
    positions = jax.random.randint(part_keys[3], (BATCH,), 0, SEQ_LEN, jnp.int32)
    positions = positions.at[0].set(SEQ_LEN - 1)
    return {
        'tokens': tokens.astype(jnp.bfloat16),
        'w_query': w_query.astype(jnp.bfloat16),
        'w_key': w_key.astype(jnp.bfloat16),
        'w_value': w_value.astype(jnp.bfloat16),
        'w_out': w_out.astype(jnp.bfloat16),
        'k_cache': k_cache.astype(jnp.bfloat16),
        'v_cache': v_cache.astype(jnp.bfloat16),
        'positions': positions,
    }


def reference(tokens, w_query, w_key, w_value, w_out, k_cache, v_cache, positions):
    groups = N_HEADS // N_KV
    query = jnp.dot(tokens, w_query, preferred_element_type=jnp.float32).astype(jnp.bfloat16)
    new_key = jnp.dot(tokens, w_key, preferred_element_type=jnp.float32).astype(jnp.bfloat16)
    new_value = jnp.dot(tokens, w_value, preferred_element_type=jnp.float32).astype(jnp.bfloat16)
    query = query.reshape(BATCH, N_KV, groups, HEAD_DIM)
    new_key = new_key.reshape(BATCH, N_KV, HEAD_DIM)
    new_value = new_value.reshape(BATCH, N_KV, HEAD_DIM)
    slot_ids = jnp.arange(SEQ_LEN, dtype=jnp.int32)

    def one_row(row_inputs):
        q_row, key_row, value_row, k_rows, v_rows, pos_row = row_inputs
        is_slot = (slot_ids == pos_row)[:, None, None]
        k_new = jnp.where(is_slot, key_row[None], k_rows)
        v_new = jnp.where(is_slot, value_row[None], v_rows)
        scores = jnp.einsum('kgd,tkd->kgt', q_row.astype(jnp.float32), k_new.astype(jnp.float32)) * HEAD_DIM ** -0.5
        scores = jnp.where(slot_ids <= pos_row, scores, -jnp.inf)
        row_max = jnp.max(scores, axis=-1, keepdims=True)
        weights = jnp.exp(scores - row_max)
        row_sum = jnp.sum(weights, axis=-1, keepdims=True)
        mixed_sum = jnp.einsum('kgt,tkd->kgd', weights.astype(jnp.bfloat16).astype(jnp.float32), v_new.astype(jnp.float32))
        attn_row = (mixed_sum / row_sum).astype(jnp.bfloat16)
        return k_new, v_new, attn_row

    k_out, v_out, attn_rows = lax.map(one_row, (query, new_key, new_value, k_cache, v_cache, positions))
    attn_flat = attn_rows.reshape(BATCH, N_HEADS * HEAD_DIM)
    y_out = jnp.dot(attn_flat, w_out, preferred_element_type=jnp.float32).astype(jnp.bfloat16)
    return y_out, k_out, v_out
```

```python
import functools

import jax
import jax.numpy as jnp
from jax import lax
from jax.experimental import pallas as pl
from jax.experimental.pallas import tpu as pltpu
from jax.sharding import PartitionSpec as P

MESH = pl.DeviceIdType.MESH
RING = 12
AHEAD = 8
PARTS = 4
F32 = jnp.float32
BF16 = jnp.bfloat16
NT = (((1,), (1,)), ((), ()))


def _at(h, s):
    return {"head": h, "seq": s}


def _greet(peers):
    barrier = pltpu.get_barrier_semaphore()
    for peer in peers:
        pl.semaphore_signal(barrier, inc=1, device_id=peer, device_id_type=MESH)
    return lambda: pl.semaphore_wait(barrier, len(peers))


def project_kernel(x_ref, wq_ref, wk_ref, wv_ref, k_hbm, v_hbm,
                   qkv_ref, kring, vring,
                   wbuf, held, wsem, ringsem, ssem, rsem):
    nseq = held.shape[0]
    h, s = lax.axis_index("head"), lax.axis_index("seq")
    cols = wbuf.shape[-1]
    rows = wbuf.shape[2]
    first = pl.multiple_of((h * nseq + s) * cols, 128)
    peers = [lax.rem(s + d, nseq) for d in range(1, nseq)]
    joined = _greet([_at(h, p) for p in peers])
    loads = []
    for j, w in enumerate((wq_ref, wk_ref, wv_ref)):
        for p in range(PARTS):
            c = pltpu.make_async_copy(
                w.at[pl.ds(p * rows, rows), pl.ds(first, cols)], wbuf.at[j, p], wsem.at[j, p])
            c.start()
            loads.append(c)
    ring = []
    for b in range(AHEAD):
        for i, (src, dst) in enumerate(((k_hbm, kring), (v_hbm, vring))):
            c = pltpu.make_async_copy(src.at[b], dst.at[b], ringsem.at[i, b])
            c.start()
            ring.append(c)
    for j in range(3):
        acc = None
        for p in range(PARTS):
            loads[j * PARTS + p].wait()
            part = jnp.dot(x_ref[:, p * rows:(p + 1) * rows], wbuf[j, p], preferred_element_type=F32)
            acc = part if acc is None else acc + part
        held[s, j] = acc.astype(BF16)
    joined()
    sends = []
    for i, p in enumerate(peers):
        c = pltpu.make_async_remote_copy(
            src_ref=held.at[s], dst_ref=held.at[s], send_sem=ssem.at[i], recv_sem=rsem.at[i],
            device_id=_at(h, p), device_id_type=MESH)
        c.start()
        sends.append(c)

    def spread(src):
        per = cols // 256
        for j in range(3):
            for i in range(per):
                for half in range(2):
                    val = held[src, j, :, i * 256 + half * 128:i * 256 + half * 128 + 128].astype(F32)
                    qkv_ref[j, half, pl.ds(src * per + i, val.shape[0], stride=nseq * per), :] = val

    spread(s)
    for i in range(nseq - 1):
        sends[i].wait_recv()
        spread(lax.rem(s + nseq - 1 - i, nseq))
    for c in sends:
        c.wait_send()
    for c in ring:
        c.wait()


def attend_kernel(scale, pos_ref, qkv_ref, k_hbm, v_hbm, kring_in, vring_in,
                  ko_hbm, vo_hbm, part_ref, stat_ref, kring, vring,
                  obuf, mbuf, lbuf, kin, vin, kout, vout):
    batch, wide, hd = k_hbm.shape
    heads = part_ref.shape[0]
    span = wide // heads
    base = lax.axis_index("seq") * span
    col = lax.broadcasted_iota(jnp.int32, (heads, wide), 1)
    row = lax.broadcasted_iota(jnp.int32, (heads, wide), 0)
    own = lax.rem(col, heads) == row
    slot_of = base + col // heads

    def fresh(j, lines):
        return jnp.concatenate([qkv_ref[j, 0, lines, :], qkv_ref[j, 1, lines, :]], axis=-1).astype(BF16)

    def body(b, carry):
        slot = lax.rem(b, RING)
        nxt = b + AHEAD

        @pl.when(nxt < batch)
        def _():
            ns = lax.rem(nxt, RING)

            @pl.when(nxt >= RING)
            def _():
                pltpu.make_async_copy(kring.at[ns], ko_hbm.at[nxt - RING], kout.at[ns]).wait()
                pltpu.make_async_copy(vring.at[ns], vo_hbm.at[nxt - RING], vout.at[ns]).wait()

            pltpu.make_async_copy(k_hbm.at[nxt], kring.at[ns], kin.at[ns]).start()
            pltpu.make_async_copy(v_hbm.at[nxt], vring.at[ns], vin.at[ns]).start()

        pos = pos_ref[b]
        at = pos - base
        mine = jnp.logical_and(at >= 0, at < span)
        lines = pl.ds(pl.multiple_of(b * heads, heads), heads)
        spot = pl.ds(pl.multiple_of(at * heads, heads), heads)

        @pl.when(b >= AHEAD)
        def _():
            pltpu.make_async_copy(k_hbm.at[b], kring.at[slot], kin.at[slot]).wait()

        @pl.when(mine)
        def _():
            kring[slot, spot, :] = fresh(1, lines)

        query = fresh(0, lines)
        keys = kring[slot]
        score = lax.dot_general(query, keys, NT, preferred_element_type=F32) * scale
        pltpu.make_async_copy(kring.at[slot], ko_hbm.at[b], kout.at[slot]).start()
        score = jnp.where(jnp.logical_and(own, slot_of <= pos), score, -jnp.inf)
        top = jnp.max(score, axis=-1, keepdims=True)
        safe = jnp.where(top == -jnp.inf, 0.0, top)
        weight = jnp.exp(score - safe)
        total = jnp.sum(weight, axis=-1, keepdims=True)

        @pl.when(b >= AHEAD)
        def _():
            pltpu.make_async_copy(v_hbm.at[b], vring.at[slot], vin.at[slot]).wait()

        @pl.when(mine)
        def _():
            vring[slot, spot, :] = fresh(2, lines)

        values = vring[slot]
        mix = jnp.dot(weight.astype(BF16), values, preferred_element_type=F32)
        obuf[0, lines, :] = mix[:, :128]
        obuf[1, lines, :] = mix[:, 128:]
        pltpu.make_async_copy(vring.at[slot], vo_hbm.at[b], vout.at[slot]).start()
        mbuf[lines, :] = jnp.broadcast_to(top, (heads, 128))
        lbuf[lines, :] = jnp.broadcast_to(total, (heads, 128))
        return carry

    lax.fori_loop(0, batch, body, 0)
    eye = (lax.broadcasted_iota(jnp.int32, (batch, 128), 0)
           == lax.broadcasted_iota(jnp.int32, (batch, 128), 1))
    for hh in range(heads):
        pick = pl.ds(hh, batch, stride=heads)
        part_ref[hh, :, :128] = obuf[0, pick, :]
        part_ref[hh, :, 128:] = obuf[1, pick, :]
        stat_ref[hh, 0:1, :] = jnp.sum(jnp.where(eye, mbuf[pick, :], 0.0), axis=0, keepdims=True)
        stat_ref[hh, 1:2, :] = jnp.sum(jnp.where(eye, lbuf[pick, :], 0.0), axis=0, keepdims=True)
    def drain(i, carry):
        b = batch - RING + i
        ns = lax.rem(b, RING)
        pltpu.make_async_copy(kring.at[ns], ko_hbm.at[b], kout.at[ns]).wait()
        pltpu.make_async_copy(vring.at[ns], vo_hbm.at[b], vout.at[ns]).wait()
        return carry

    lax.fori_loop(0, RING, drain, 0)


def finish_kernel(part_ref, stat_ref, wo_hbm, y_ref,
                  gpart, gstat, wo, ysend, ygot, yout,
                  wsem, s1, r1, s2, r2, s3, r3, s4, r4):
    nseq = gpart.shape[0]
    per, batch, hd = gpart.shape[1:]
    ndev = ysend.shape[0]
    cols = ysend.shape[-1]
    h, s = lax.axis_index("head"), lax.axis_index("seq")
    me = h * nseq + s
    far = [lax.rem(me + d, ndev) for d in range(1, ndev)]
    joined = _greet([_at(p // nseq, lax.rem(p, nseq)) for p in far])
    load = pltpu.make_async_copy(wo_hbm, wo, wsem)
    load.start()
    joined()
    near = [lax.rem(s + d, nseq) for d in range(1, nseq)]
    sends = []
    for i, p in enumerate(near):
        c = pltpu.make_async_remote_copy(
            src_ref=part_ref.at[pl.ds(p * per, per)], dst_ref=gpart.at[i], send_sem=s1.at[i],
            recv_sem=r1.at[i], device_id=_at(h, p), device_id_type=MESH)
        d = pltpu.make_async_remote_copy(
            src_ref=stat_ref.at[pl.ds(p * per, per)], dst_ref=gstat.at[i], send_sem=s4.at[i],
            recv_sem=r4.at[i], device_id=_at(h, p), device_id_type=MESH)
        c.start()
        d.start()
        sends += [c, d]
    for c in sends:
        c.wait_recv()
    eye = (lax.broadcasted_iota(jnp.int32, (batch, 128), 0)
           == lax.broadcasted_iota(jnp.int32, (batch, 128), 1))
    y = None
    load.wait()
    for e in range(per):
        mine = stat_ref[s * per + e]
        stats = [mine] + [gstat[i, e] for i in range(nseq - 1)]
        parts = [part_ref[s * per + e]] + [gpart[i, e] for i in range(nseq - 1)]
        top = functools.reduce(jnp.maximum, [t[0:1] for t in stats])
        mix, total = None, None
        for t, part in zip(stats, parts):
            factor = jnp.exp(t[0:1] - top)
            line = factor * t[1:2]
            total = line if total is None else total + line
            down = jnp.sum(jnp.where(eye, factor, 0.0), axis=1, keepdims=True)
            mix = part * down if mix is None else mix + part * down
        down = jnp.sum(jnp.where(eye, total, 0.0), axis=1, keepdims=True)
        attn = (mix / down).astype(BF16)
        term = jnp.dot(attn, wo[e * hd:(e + 1) * hd, :], preferred_element_type=F32)
        y = term if y is None else y + term
    for p in range(ndev):
        ysend[p] = y[:, p * cols:(p + 1) * cols]
    moves = []
    for i, p in enumerate(far):
        c = pltpu.make_async_remote_copy(
            src_ref=ysend.at[p], dst_ref=ygot.at[i], send_sem=s2.at[i], recv_sem=r2.at[i],
            device_id=_at(p // nseq, lax.rem(p, nseq)), device_id_type=MESH)
        c.start()
        moves.append(c)
    acc = ysend[me]
    for i, c in enumerate(moves):
        c.wait_recv()
        acc = acc + ygot[i]
    yout[me] = acc.astype(BF16)
    shares = []
    for i, p in enumerate(far):
        c = pltpu.make_async_remote_copy(
            src_ref=yout.at[me], dst_ref=yout.at[me], send_sem=s3.at[i], recv_sem=r3.at[i],
            device_id=_at(p // nseq, lax.rem(p, nseq)), device_id_type=MESH)
        c.start()
        shares.append(c)
    for c in shares:
        c.wait_recv()
    for p in range(ndev):
        y_ref[:, p * cols:(p + 1) * cols] = yout[p]
    for c in sends + moves + shares:
        c.wait_send()


def solution(mesh):
    nhead, nseq = mesh.shape["head"], mesh.shape["seq"]
    ndev = nhead * nseq
    cache_spec = P("rep", "seq", "head", None)
    any_spec = pl.BlockSpec(memory_space=pl.ANY)
    vmem = pl.BlockSpec(memory_space=pltpu.VMEM)
    smem = pl.BlockSpec(memory_space=pltpu.SMEM)

    def local_step(tokens, w_query, w_key, w_value, w_out, k_cache, v_cache, positions):
        batch, span, heads, hd = k_cache.shape
        model = tokens.shape[1]
        cols = heads * hd // nseq
        per = heads // nseq
        ring = jax.ShapeDtypeStruct((RING, span * heads, hd), BF16)
        cache = jax.ShapeDtypeStruct((batch, span * heads, hd), BF16)
        k_flat, v_flat = k_cache.reshape(cache.shape), v_cache.reshape(cache.shape)
        dma = pltpu.SemaphoreType.DMA
        qkv, kring, vring = pl.pallas_call(
            project_kernel,
            out_shape=(jax.ShapeDtypeStruct((3, 2, batch * heads, 128), F32), ring, ring),
            in_specs=[vmem] + [any_spec] * 5,
            out_specs=(vmem, vmem, vmem),
            scratch_shapes=[
                pltpu.VMEM((3, PARTS, model // PARTS, cols), BF16),
                pltpu.VMEM((nseq, 3, batch, cols), BF16),
                dma((3, PARTS)), dma((2, AHEAD)), dma((nseq - 1,)), dma((nseq - 1,)),
            ],
            compiler_params=pltpu.CompilerParams(
                collective_id=0, has_side_effects=True, vmem_limit_bytes=14 * 2**20),
        )(tokens, w_query, w_key, w_value, k_flat, v_flat)
        k_out, v_out, part, stat, _, _ = pl.pallas_call(
            functools.partial(attend_kernel, hd ** -0.5),
            out_shape=(cache, cache, jax.ShapeDtypeStruct((heads, batch, hd), F32),
                       jax.ShapeDtypeStruct((heads, 8, 128), F32), ring, ring),
            in_specs=[smem, vmem, any_spec, any_spec, vmem, vmem],
            out_specs=(any_spec, any_spec, vmem, vmem, vmem, vmem),
            input_output_aliases={4: 4, 5: 5},
            scratch_shapes=[
                pltpu.VMEM((2, batch * heads, 128), F32),
                pltpu.VMEM((batch * heads, 128), F32),
                pltpu.VMEM((batch * heads, 128), F32),
                dma((RING,)), dma((RING,)), dma((RING,)), dma((RING,)),
            ],
            compiler_params=pltpu.CompilerParams(vmem_limit_bytes=8 * 2**20),
        )(positions, qkv, k_flat, v_flat, kring, vring)
        ycols = model // ndev
        y = pl.pallas_call(
            finish_kernel,
            out_shape=jax.ShapeDtypeStruct((batch, model), BF16),
            in_specs=[vmem, vmem, any_spec],
            out_specs=vmem,
            scratch_shapes=[
                pltpu.VMEM((nseq, per, batch, hd), F32),
                pltpu.VMEM((nseq, per, 8, 128), F32),
                pltpu.VMEM(w_out.shape, BF16),
                pltpu.VMEM((ndev, batch, ycols), F32),
                pltpu.VMEM((ndev, batch, ycols), F32),
                pltpu.VMEM((ndev, batch, ycols), BF16),
                dma, dma((nseq,)), dma((nseq,)), dma((ndev,)), dma((ndev,)),
                dma((ndev,)), dma((ndev,)), dma((nseq,)), dma((nseq,)),
            ],
            compiler_params=pltpu.CompilerParams(
                collective_id=1, has_side_effects=True, vmem_limit_bytes=12 * 2**20),
        )(part, stat, w_out)
        return y, k_out.reshape(k_cache.shape), v_out.reshape(v_cache.shape)

    return jax.shard_map(
        local_step,
        mesh=mesh,
        in_specs=(P("rep", None), P(), P(), P(), P(("head", "seq"), None), cache_spec, cache_spec, P("rep")),
        out_specs=(P("rep", None), cache_spec, cache_spec),
        check_vma=False,
    )
```

```python
import functools

import jax
import jax.numpy as jnp
from jax import lax
from jax.experimental import pallas as pl
from jax.experimental.pallas import tpu as pltpu
from jax.sharding import PartitionSpec as P

MESH = pl.DeviceIdType.MESH
RING = 16
AHEAD = 9
PARTS = 4
SPLITS = (21, 27)
F32 = jnp.float32
BF16 = jnp.bfloat16
NT = (((1,), (1,)), ((), ()))


def _at(h, s):
    return {"head": h, "seq": s}


def _greet(peers):
    barrier = pltpu.get_barrier_semaphore()
    for peer in peers:
        pl.semaphore_signal(barrier, inc=1, device_id=peer, device_id_type=MESH)
    return lambda: pl.semaphore_wait(barrier, len(peers))


def project_kernel(x_ref, wq_ref, wk_ref, wv_ref, k_hbm, v_hbm,
                   qkv_ref, kring, vring,
                   wbuf, held, wsem, ringsem, ssem, rsem):
    nseq = held.shape[0]
    h, s = lax.axis_index("head"), lax.axis_index("seq")
    cols = wbuf.shape[-1]
    rows = wbuf.shape[2]
    first = pl.multiple_of((h * nseq + s) * cols, 128)
    peers = [lax.rem(s + d, nseq) for d in range(1, nseq)]
    joined = _greet([_at(h, p) for p in peers])
    loads = []
    for j, w in enumerate((wq_ref, wk_ref, wv_ref)):
        for p in range(PARTS):
            c = pltpu.make_async_copy(
                w.at[pl.ds(p * rows, rows), pl.ds(first, cols)], wbuf.at[j, p], wsem.at[j, p])
            c.start()
            loads.append(c)
    ring = []
    for b in range(AHEAD):
        for i, (src, dst) in enumerate(((k_hbm, kring), (v_hbm, vring))):
            ring.append(pltpu.make_async_copy(src.at[b], dst.at[b], ringsem.at[i, b]))
    asked = 0
    sends = []
    for j in range(3):
        acc = None
        for p in range(PARTS):
            loads[j * PARTS + p].wait()
            share = -(-len(ring) * (j * PARTS + p + 1) // (3 * PARTS))
            while asked < share:
                ring[asked].start()
                asked += 1
            part = jnp.dot(x_ref[:, p * rows:(p + 1) * rows], wbuf[j, p], preferred_element_type=F32)
            acc = part if acc is None else acc + part
        held[s, j] = acc.astype(BF16)
        if j == 0:
            joined()
        for i, p in enumerate(peers):
            c = pltpu.make_async_remote_copy(
                src_ref=held.at[s, j], dst_ref=held.at[s, j], send_sem=ssem.at[j, i], recv_sem=rsem.at[j, i],
                device_id=_at(h, p), device_id_type=MESH)
            c.start()
            sends.append(c)

    def spread(src, which):
        per = cols // 256
        for j in which:
            for i in range(per):
                for half in range(2):
                    val = held[src, j, :, i * 256 + half * 128:i * 256 + half * 128 + 128].astype(F32)
                    qkv_ref[j, half, pl.ds(src * per + i, val.shape[0], stride=nseq * per), :] = val

    spread(s, range(3))
    for j in range(3):
        for i in range(nseq - 1):
            sends[j * (nseq - 1) + i].wait_recv()
            spread(lax.rem(s + nseq - 1 - i, nseq), (j,))
    for c in sends:
        c.wait_send()
    for c in ring:
        c.wait()


def attend_kernel(scale, pos_ref, qkv_ref, k_hbm, v_hbm, kring_in, vring_in,
                  ko_hbm, vo_hbm, kring, vring, *rest):
    chunks = rest[:-7]
    attend_body(scale, pos_ref, qkv_ref, k_hbm, v_hbm, ko_hbm, vo_hbm, kring, vring, chunks, *rest[-7:])


def attend_body(scale, pos_ref, qkv_ref, k_hbm, v_hbm, ko_hbm, vo_hbm, kring, vring, chunks,
                  obuf, mbuf, lbuf, kin, vin, kout, vout):
    batch, wide, hd = k_hbm.shape
    nseq = len(chunks)
    heads = obuf.shape[1] // batch
    per = heads // nseq
    span = wide // heads
    base = lax.axis_index("seq") * span
    col = lax.broadcasted_iota(jnp.int32, (heads, wide), 1)
    row = lax.broadcasted_iota(jnp.int32, (heads, wide), 0)
    own = lax.rem(col, heads) == row
    slot_of = base + col // heads

    def fresh(j, lines):
        return jnp.concatenate([qkv_ref[j, 0, lines, :], qkv_ref[j, 1, lines, :]], axis=-1).astype(BF16)

    def body(b, carry):
        slot = lax.rem(b, RING)
        nxt = b + AHEAD

        @pl.when(nxt < batch)
        def _():
            ns = lax.rem(nxt, RING)

            @pl.when(nxt >= RING)
            def _():
                pltpu.make_async_copy(kring.at[ns], ko_hbm.at[nxt - RING], kout.at[ns]).wait()
                pltpu.make_async_copy(vring.at[ns], vo_hbm.at[nxt - RING], vout.at[ns]).wait()

            pltpu.make_async_copy(k_hbm.at[nxt], kring.at[ns], kin.at[ns]).start()
            pltpu.make_async_copy(v_hbm.at[nxt], vring.at[ns], vin.at[ns]).start()

        pos = pos_ref[b]
        at = pos - base
        mine = jnp.logical_and(at >= 0, at < span)
        lines = pl.ds(pl.multiple_of(b * heads, heads), heads)
        spot = pl.ds(pl.multiple_of(at * heads, heads), heads)

        @pl.when(b >= AHEAD)
        def _():
            pltpu.make_async_copy(k_hbm.at[b], kring.at[slot], kin.at[slot]).wait()

        @pl.when(mine)
        def _():
            kring[slot, spot, :] = fresh(1, lines)

        query = fresh(0, lines)
        keys = kring[slot]
        score = lax.dot_general(query, keys, NT, preferred_element_type=F32) * scale

        @pl.when(b < batch - RING)
        def _():
            pltpu.make_async_copy(kring.at[slot], ko_hbm.at[b], kout.at[slot]).start()

        score = jnp.where(jnp.logical_and(own, slot_of <= pos), score, -jnp.inf)
        top = jnp.max(score, axis=-1, keepdims=True)
        safe = jnp.where(top == -jnp.inf, 0.0, top)
        weight = jnp.exp(score - safe)
        total = jnp.sum(weight, axis=-1, keepdims=True)

        @pl.when(b >= AHEAD)
        def _():
            pltpu.make_async_copy(v_hbm.at[b], vring.at[slot], vin.at[slot]).wait()

        @pl.when(mine)
        def _():
            vring[slot, spot, :] = fresh(2, lines)

        values = vring[slot]
        mix = jnp.dot(weight.astype(BF16), values, preferred_element_type=F32)
        obuf[0, lines, :] = mix[:, :128]
        obuf[1, lines, :] = mix[:, 128:]

        @pl.when(b < batch - RING)
        def _():
            pltpu.make_async_copy(vring.at[slot], vo_hbm.at[b], vout.at[slot]).start()

        mbuf[lines, :] = jnp.broadcast_to(top, (heads, 128))
        lbuf[lines, :] = jnp.broadcast_to(total, (heads, 128))
        return carry

    lax.fori_loop(0, batch, body, 0)
    eye = (lax.broadcasted_iota(jnp.int32, (batch, 128), 0)
           == lax.broadcasted_iota(jnp.int32, (batch, 128), 1))
    me = lax.axis_index("seq")
    for d, chunk in enumerate(chunks):
        for e in range(per):
            pick = pl.ds(lax.rem(me + d, nseq) * per + e, batch, stride=heads)
            rows = slice(e * batch, (e + 1) * batch)
            chunk[rows, :128] = obuf[0, pick, :]
            chunk[rows, 128:] = obuf[1, pick, :]
            for i, buf in enumerate((mbuf, lbuf)):
                line = per * batch + 2 * e + i
                chunk[line:line + 1, :128] = jnp.sum(jnp.where(eye, buf[pick, :], 0.0), axis=0, keepdims=True)
                chunk[line:line + 1, 128:] = jnp.zeros((1, hd - 128), F32)
        used = per * batch + 2 * per
        chunk[used:, :] = jnp.zeros((chunk.shape[0] - used, hd), F32)


def write_kernel(lo, hi, kring, vring, ko_in, vo_in, after, ko_hbm, vo_hbm, done, sem):
    copies = []
    for b in range(lo, hi):
        for src, dst in ((kring, ko_hbm), (vring, vo_hbm)):
            c = pltpu.make_async_copy(src.at[b % RING], dst.at[b], sem.at[len(copies)])
            c.start()
            copies.append(c)
    done[...] = jnp.zeros_like(done)
    for c in copies:
        c.wait()


def combine_kernel(ndev, own, *refs):
    refs = list(refs)
    nrecv = len(refs) - 2 - ndev - 1
    got, (wo, after) = refs[:nrecv], refs[nrecv:nrecv + 2]
    outs, ybuf = refs[nrecv + 2:-1], refs[-1]
    chunks = [own] + got
    nseq = len(chunks)
    batch, cols = outs[0].shape
    per = (own.shape[0] - 8) // batch
    hd = own.shape[1]
    h, s = lax.axis_index("head"), lax.axis_index("seq")
    me = h * nseq + s
    eye = (lax.broadcasted_iota(jnp.int32, (batch, hd), 0)
           == lax.broadcasted_iota(jnp.int32, (batch, hd), 1))
    y = None
    for e in range(per):
        tops = [c[per * batch + 2 * e:per * batch + 2 * e + 1, :] for c in chunks]
        sums = [c[per * batch + 2 * e + 1:per * batch + 2 * e + 2, :] for c in chunks]
        top = functools.reduce(jnp.maximum, tops)
        mix, total = None, None
        for c, t, l in zip(chunks, tops, sums):
            factor = jnp.exp(t - top)
            line = factor * l
            total = line if total is None else total + line
            down = jnp.sum(jnp.where(eye, factor, 0.0), axis=1, keepdims=True)
            term = c[e * batch:(e + 1) * batch, :] * down
            mix = term if mix is None else mix + term
        down = jnp.sum(jnp.where(eye, total, 0.0), axis=1, keepdims=True)
        attn = (mix / down).astype(BF16)
        term = jnp.dot(attn, wo[e * hd:(e + 1) * hd, :], preferred_element_type=F32)
        y = term if y is None else y + term
    for p in range(ndev):
        ybuf[p] = y[:, p * cols:(p + 1) * cols]
    for d in range(ndev):
        outs[d][...] = ybuf[lax.rem(me + d, ndev)]


def total_kernel(*refs):
    out = refs[-1]
    acc = refs[0][...]
    for r in refs[1:-2]:
        acc = acc + r[...]
    out[...] = acc.astype(BF16)


def gather_kernel(nseq, *refs):
    out = refs[-1]
    blocks = refs[:-2]
    ndev = len(blocks)
    cols = blocks[0].shape[1]
    me = lax.axis_index("head") * nseq + lax.axis_index("seq")
    for d, blk in enumerate(blocks):
        src = lax.rem(me + ndev - d, ndev)
        out[:, pl.ds(pl.multiple_of(src * cols, 128), cols)] = blk[...]


def solution(mesh):
    nhead, nseq = mesh.shape["head"], mesh.shape["seq"]
    ndev = nhead * nseq
    cache_spec = P("rep", "seq", "head", None)
    any_spec = pl.BlockSpec(memory_space=pl.ANY)
    vmem = pl.BlockSpec(memory_space=pltpu.VMEM)
    smem = pl.BlockSpec(memory_space=pltpu.SMEM)

    def local_step(tokens, w_query, w_key, w_value, w_out, k_cache, v_cache, positions):
        batch, span, heads, hd = k_cache.shape
        model = tokens.shape[1]
        cols = heads * hd // nseq
        per = heads // nseq
        ring = jax.ShapeDtypeStruct((RING, span * heads, hd), BF16)
        cache = jax.ShapeDtypeStruct((batch, span * heads, hd), BF16)
        k_flat, v_flat = k_cache.reshape(cache.shape), v_cache.reshape(cache.shape)
        dma = pltpu.SemaphoreType.DMA
        qkv, kring, vring = pl.pallas_call(
            project_kernel,
            out_shape=(jax.ShapeDtypeStruct((3, 2, batch * heads, 128), F32), ring, ring),
            in_specs=[vmem] + [any_spec] * 5,
            out_specs=(vmem, vmem, vmem),
            scratch_shapes=[
                pltpu.VMEM((3, PARTS, model // PARTS, cols), BF16),
                pltpu.VMEM((nseq, 3, batch, cols), BF16),
                dma((3, PARTS)), dma((2, AHEAD)), dma((3, nseq - 1)), dma((3, nseq - 1)),
            ],
            compiler_params=pltpu.CompilerParams(
                collective_id=0, has_side_effects=True, vmem_limit_bytes=11 * 2**20),
        )(tokens, w_query, w_key, w_value, k_flat, v_flat)
        chunk = jax.ShapeDtypeStruct((per * batch + 8, hd), F32)
        k_out, v_out, kring, vring, *chunks = pl.pallas_call(
            functools.partial(attend_kernel, hd ** -0.5),
            out_shape=(cache, cache, ring, ring) + (chunk,) * nseq,
            in_specs=[smem, vmem, any_spec, any_spec, vmem, vmem],
            out_specs=(any_spec, any_spec, vmem, vmem) + (vmem,) * nseq,
            input_output_aliases={4: 2, 5: 3},
            scratch_shapes=[
                pltpu.VMEM((2, batch * heads, 128), F32),
                pltpu.VMEM((batch * heads, 128), F32),
                pltpu.VMEM((batch * heads, 128), F32),
                dma((RING,)), dma((RING,)), dma((RING,)), dma((RING,)),
            ],
            compiler_params=pltpu.CompilerParams(vmem_limit_bytes=4 * 2**20),
        )(positions, qkv, k_flat, v_flat, kring, vring)

        mark = jax.ShapeDtypeStruct((8, 128), F32)

        def write(k_out, v_out, lo, hi, after):
            return pl.pallas_call(
                functools.partial(write_kernel, lo, hi),
                out_shape=(cache, cache, mark),
                in_specs=[vmem, vmem, any_spec, any_spec, vmem],
                out_specs=(any_spec, any_spec, vmem),
                input_output_aliases={2: 0, 3: 1},
                scratch_shapes=[dma((2 * (hi - lo),))],
                compiler_params=pltpu.CompilerParams(vmem_limit_bytes=1 * 2**20),
                cost_estimate=pl.CostEstimate(flops=10**8 * (hi - lo), bytes_accessed=2 * (hi - lo) * 2**20, transcendentals=0),
            )(kring, vring, k_out, v_out, after)

        def turn(x, axes, n, d):
            return lax.ppermute(x, axes, [(i, (i + d) % n) for i in range(n)])

        both = ("head", "seq")
        ycols = model // ndev
        block = jax.ShapeDtypeStruct((batch, ycols), F32)
        got = [turn(chunks[d], "seq", nseq, d) for d in range(1, nseq)]
        k_out, v_out, after = write(k_out, v_out, batch - RING, SPLITS[0], chunks[0])
        blocks = pl.pallas_call(
            functools.partial(combine_kernel, ndev),
            out_shape=(block,) * ndev,
            in_specs=[vmem] * (nseq + 2),
            out_specs=(vmem,) * ndev,
            scratch_shapes=[pltpu.VMEM((ndev, batch, ycols), F32)],
            compiler_params=pltpu.CompilerParams(vmem_limit_bytes=4 * 2**20),
        )(chunks[0], *got, w_out, after)
        terms = [turn(blocks[d], both, ndev, d) for d in range(1, ndev)]
        k_out, v_out, after = write(k_out, v_out, SPLITS[0], SPLITS[1], blocks[0])
        mine = pl.pallas_call(
            total_kernel,
            out_shape=jax.ShapeDtypeStruct((batch, ycols), BF16),
            in_specs=[vmem] * (ndev + 1),
            out_specs=vmem,
            compiler_params=pltpu.CompilerParams(vmem_limit_bytes=2 * 2**20),
        )(blocks[0], *terms, after)
        pieces = [turn(mine, both, ndev, d) for d in range(1, ndev)]
        k_out, v_out, after = write(k_out, v_out, SPLITS[1], batch, mine)
        y = pl.pallas_call(
            functools.partial(gather_kernel, nseq),
            out_shape=jax.ShapeDtypeStruct((batch, model), BF16),
            in_specs=[vmem] * (ndev + 1),
            out_specs=vmem,
            compiler_params=pltpu.CompilerParams(vmem_limit_bytes=2 * 2**20),
        )(mine, *pieces, after)
        return y, k_out.reshape(k_cache.shape), v_out.reshape(v_cache.shape)

    return jax.shard_map(
        local_step,
        mesh=mesh,
        in_specs=(P("rep", None), P(), P(), P(), P(("head", "seq"), None), cache_spec, cache_spec, P("rep")),
        out_specs=(P("rep", None), cache_spec, cache_spec),
        check_vma=False,
    )
```

```python
import functools

import jax
import jax.numpy as jnp
from jax import lax
from jax.experimental import pallas as pl
from jax.experimental.pallas import tpu as pltpu
from jax.sharding import PartitionSpec as P

MESH = pl.DeviceIdType.MESH
RING = 6
AHEAD = 4
HELD = 4
PARTS = 4
F32 = jnp.float32
BF16 = jnp.bfloat16
NT = (((1,), (1,)), ((), ()))


def _at(h, s):
    return {"head": h, "seq": s}


def _greet(peers):
    barrier = pltpu.get_barrier_semaphore()
    for peer in peers:
        pl.semaphore_signal(barrier, inc=1, device_id=peer, device_id_type=MESH)
    return lambda: pl.semaphore_wait(barrier, len(peers))


def project_kernel(x_hbm, wq_ref, wk_ref, wv_ref, k_hbm, v_hbm,
                   qkv_ref, kring, vring,
                   x_ref, wbuf, held, xsem, wsem, ringsem, ssem, rsem):
    nseq = held.shape[0]
    h, s = lax.axis_index("head"), lax.axis_index("seq")
    cols = wbuf.shape[-1]
    rows = wbuf.shape[2]
    first = pl.multiple_of((h * nseq + s) * cols, 128)
    peers = [lax.rem(s + d, nseq) for d in range(1, nseq)]
    joined = _greet([_at(h, p) for p in peers])
    tokens = pltpu.make_async_copy(x_hbm, x_ref, xsem)
    tokens.start()
    loads = []
    for j, w in enumerate((wq_ref, wk_ref, wv_ref)):
        for p in range(PARTS):
            c = pltpu.make_async_copy(
                w.at[pl.ds(p * rows, rows), pl.ds(first, cols)], wbuf.at[j, p], wsem.at[j, p])
            c.start()
            loads.append(c)
    ring = []
    for b in range(AHEAD):
        for i, (src, dst) in enumerate(((k_hbm, kring), (v_hbm, vring))):
            pair = pl.ds(2 * b, 2)
            ring.append(pltpu.make_async_copy(src.at[pair], dst.at[pair], ringsem.at[i, b]))
    asked = 0
    sends = []
    tokens.wait()
    for j in range(3):
        acc = None
        for p in range(PARTS):
            loads[j * PARTS + p].wait()
            share = -(-len(ring) * (j * PARTS + p + 1) // (3 * PARTS))
            while asked < share:
                ring[asked].start()
                asked += 1
            part = jnp.dot(x_ref[:, p * rows:(p + 1) * rows], wbuf[j, p], preferred_element_type=F32)
            acc = part if acc is None else acc + part
        held[s, j] = acc.astype(BF16)
        if j == 0:
            joined()
        for i, p in enumerate(peers):
            c = pltpu.make_async_remote_copy(
                src_ref=held.at[s, j], dst_ref=held.at[s, j], send_sem=ssem.at[j, i], recv_sem=rsem.at[j, i],
                device_id=_at(h, p), device_id_type=MESH)
            c.start()
            sends.append(c)

    def spread(src, which):
        per = cols // 256
        for j in which:
            for i in range(per):
                for half in range(2):
                    val = held[src, j, :, i * 256 + half * 128:i * 256 + half * 128 + 128].astype(F32)
                    qkv_ref[j, half, pl.ds(src * per + i, val.shape[0], stride=nseq * per), :] = val

    spread(s, range(3))
    for j in range(3):
        for i in range(nseq - 1):
            sends[j * (nseq - 1) + i].wait_recv()
            spread(lax.rem(s + nseq - 1 - i, nseq), (j,))
    for c in sends:
        c.wait_send()
    for c in ring:
        c.wait()


def attend_kernel(scale, pos_ref, qkv_ref, k_hbm, v_hbm, kring_in, vring_in,
                  ko_hbm, vo_hbm, kring, vring, *rest):
    chunks = rest[:-7]
    obuf, mbuf, lbuf, kin, vin, kout, vout = rest[-7:]
    batch, wide, hd = k_hbm.shape
    nseq = len(chunks)
    heads = obuf.shape[1] // batch
    per = heads // nseq
    span = wide // heads
    pairs = batch // 2
    base = lax.axis_index("seq") * span
    col = lax.broadcasted_iota(jnp.int32, (heads, wide), 1)
    row = lax.broadcasted_iota(jnp.int32, (heads, wide), 0)
    own = lax.rem(col, heads) == row
    slot_of = jnp.where(own, base + col // heads, batch * nseq * span)

    def both(i):
        return pl.ds(pl.multiple_of(i * 2, 2), 2)

    def reads(i):
        slot = lax.rem(i, RING)
        return [pltpu.make_async_copy(src.at[both(i)], dst.at[both(slot)], sem.at[slot])
                for src, dst, sem in ((k_hbm, kring, kin), (v_hbm, vring, vin))]

    def writes(i):
        slot = lax.rem(i, RING)
        return [pltpu.make_async_copy(src.at[both(slot)], dst.at[both(i)], sem.at[slot])
                for src, dst, sem in ((kring, ko_hbm, kout), (vring, vo_hbm, vout))]

    def fresh(j, lines):
        return jnp.concatenate([qkv_ref[j, 0, lines, :], qkv_ref[j, 1, lines, :]], axis=-1).astype(BF16)

    def body(i, carry):
        nxt = i + AHEAD

        @pl.when(nxt < pairs)
        def _():
            @pl.when(nxt >= RING)
            def _():
                for c in writes(nxt - RING):
                    c.wait()

            for c in reads(nxt):
                c.start()

        @pl.when(i >= AHEAD)
        def _():
            for c in reads(i):
                c.wait()

        rows = []
        for g in range(2):
            b = 2 * i + g
            pos = pos_ref[b]
            at = pos - base
            lines = pl.ds(pl.multiple_of(b * heads, heads), heads)
            spot = pl.ds(pl.multiple_of(at * heads, heads), heads)
            ks = 2 * lax.rem(i, RING) + g

            @pl.when(jnp.logical_and(at >= 0, at < span))
            def _():
                kring[ks, spot, :] = fresh(1, lines)
                vring[ks, spot, :] = fresh(2, lines)

            rows.append((b, pos, lines, ks))
        scores = []
        for b, pos, lines, ks in rows:
            score = lax.dot_general(fresh(0, lines), kring[ks], NT, preferred_element_type=F32) * scale
            scores.append(jnp.where(slot_of <= pos, score, -jnp.inf))
        for (b, pos, lines, ks), score in zip(rows, scores):
            top = jnp.max(score, axis=-1, keepdims=True)
            safe = jnp.where(top == -jnp.inf, 0.0, top)
            weight = jnp.exp(score - safe)
            total = jnp.sum(weight, axis=-1, keepdims=True)
            mix = jnp.dot(weight.astype(BF16), vring[ks], preferred_element_type=F32)
            obuf[0, lines, :] = mix[:, :128]
            obuf[1, lines, :] = mix[:, 128:]
            mbuf[lines, :] = jnp.broadcast_to(top, (heads, 128))
            lbuf[lines, :] = jnp.broadcast_to(total, (heads, 128))

        @pl.when(i < pairs - HELD)
        def _():
            for c in writes(i):
                c.start()

        return carry

    lax.fori_loop(0, pairs, body, 0)
    eye = (lax.broadcasted_iota(jnp.int32, (batch, 128), 0)
           == lax.broadcasted_iota(jnp.int32, (batch, 128), 1))
    me = lax.axis_index("seq")
    for d, chunk in enumerate(chunks):
        for e in range(per):
            pick = pl.ds(jnp.bitwise_xor(me, d) * per + e, batch, stride=heads)
            rows = slice(e * batch, (e + 1) * batch)
            chunk[rows, :128] = obuf[0, pick, :]
            chunk[rows, 128:] = obuf[1, pick, :]
            for i, buf in enumerate((mbuf, lbuf)):
                line = per * batch + 2 * e + i
                chunk[line:line + 1, :128] = jnp.sum(jnp.where(eye, buf[pick, :], 0.0), axis=0, keepdims=True)
                chunk[line:line + 1, 128:] = jnp.zeros((1, hd - 128), F32)
        used = per * batch + 2 * per
        chunk[used:, :] = jnp.zeros((chunk.shape[0] - used, hd), F32)
    for i in range(pairs - RING, pairs - HELD):
        for c in writes(i):
            c.wait()


def write_kernel(kring, vring, ko_in, vo_in, chunk, ko_hbm, vo_hbm, done, sem):
    pairs = ko_hbm.shape[0] // 2
    copies = []
    for i in range(pairs - HELD, pairs):
        for src, dst in ((kring, ko_hbm), (vring, vo_hbm)):
            c = pltpu.make_async_copy(
                src.at[pl.ds(i % RING * 2, 2)], dst.at[pl.ds(i * 2, 2)], sem.at[len(copies)])
            c.start()
            copies.append(c)
    done[...] = jnp.zeros_like(done)
    for c in copies:
        c.wait()


def finish_kernel(*refs):
    got = refs[:-10]
    wo, after, y_ref, ysend, ygot, yout, s2, r2, s3, r3 = refs[-10:]
    nseq = len(got)
    ndev, batch, cols = ysend.shape
    hd = got[0].shape[1]
    per = (got[0].shape[0] - 8) // batch
    h, s = lax.axis_index("head"), lax.axis_index("seq")
    me = h * nseq + s
    far = [lax.rem(me + d, ndev) for d in range(1, ndev)]
    joined = _greet([_at(p // nseq, lax.rem(p, nseq)) for p in far])
    eye = (lax.broadcasted_iota(jnp.int32, (batch, hd), 0)
           == lax.broadcasted_iota(jnp.int32, (batch, hd), 1))
    y = None
    for e in range(per):
        line = per * batch + 2 * e
        tops = [got[i][line:line + 1, :] for i in range(nseq)]
        sums = [got[i][line + 1:line + 2, :] for i in range(nseq)]
        top = functools.reduce(jnp.maximum, tops)
        mix, total = None, None
        for i in range(nseq):
            factor = jnp.exp(tops[i] - top)
            share = factor * sums[i]
            total = share if total is None else total + share
            down = jnp.sum(jnp.where(eye, factor, 0.0), axis=1, keepdims=True)
            term = got[i][e * batch:(e + 1) * batch, :] * down
            mix = term if mix is None else mix + term
        down = jnp.sum(jnp.where(eye, total, 0.0), axis=1, keepdims=True)
        attn = (mix / down).astype(BF16)
        term = jnp.dot(attn, wo[e * hd:(e + 1) * hd, :], preferred_element_type=F32)
        y = term if y is None else y + term
    for p in range(ndev):
        ysend[p] = y[:, p * cols:(p + 1) * cols]
    joined()
    moves = []
    for i, p in enumerate(far):
        c = pltpu.make_async_remote_copy(
            src_ref=ysend.at[p], dst_ref=ygot.at[i], send_sem=s2.at[i], recv_sem=r2.at[i],
            device_id=_at(p // nseq, lax.rem(p, nseq)), device_id_type=MESH)
        c.start()
        moves.append(c)
    acc = ysend[me]
    for i, c in enumerate(moves):
        c.wait_recv()
        acc = acc + ygot[i]
    yout[me] = acc.astype(BF16)
    shares = []
    for i, p in enumerate(far):
        c = pltpu.make_async_remote_copy(
            src_ref=yout.at[me], dst_ref=yout.at[me], send_sem=s3.at[i], recv_sem=r3.at[i],
            device_id=_at(p // nseq, lax.rem(p, nseq)), device_id_type=MESH)
        c.start()
        shares.append(c)
    for c in shares:
        c.wait_recv()
    for p in range(ndev):
        y_ref[:, p * cols:(p + 1) * cols] = yout[p]
    for c in moves + shares:
        c.wait_send()


def solution(mesh):
    nhead, nseq = mesh.shape["head"], mesh.shape["seq"]
    ndev = nhead * nseq
    cache_spec = P("rep", "seq", "head", None)
    any_spec = pl.BlockSpec(memory_space=pl.ANY)
    vmem = pl.BlockSpec(memory_space=pltpu.VMEM)
    smem = pl.BlockSpec(memory_space=pltpu.SMEM)

    def local_step(tokens, w_query, w_key, w_value, w_out, k_cache, v_cache, positions):
        batch, span, heads, hd = k_cache.shape
        model = tokens.shape[1]
        cols = heads * hd // nseq
        per = heads // nseq
        cache = jax.ShapeDtypeStruct((batch, span * heads, hd), BF16)
        ring = jax.ShapeDtypeStruct((2 * RING, span * heads, hd), BF16)
        k_flat, v_flat = k_cache.reshape(cache.shape), v_cache.reshape(cache.shape)
        dma = pltpu.SemaphoreType.DMA
        qkv, kring, vring = pl.pallas_call(
            project_kernel,
            out_shape=(jax.ShapeDtypeStruct((3, 2, batch * heads, 128), F32), ring, ring),
            in_specs=[pl.BlockSpec(memory_space=pltpu.HBM)] + [any_spec] * 5,
            out_specs=(vmem, vmem, vmem),
            scratch_shapes=[
                pltpu.VMEM(tokens.shape, BF16),
                pltpu.VMEM((3, PARTS, model // PARTS, cols), BF16),
                pltpu.VMEM((nseq, 3, batch, cols), BF16),
                dma, dma((3, PARTS)), dma((2, AHEAD)), dma((3, nseq - 1)), dma((3, nseq - 1)),
            ],
            compiler_params=pltpu.CompilerParams(
                collective_id=0, has_side_effects=True, vmem_limit_bytes=11 * 2**20),
        )(tokens, w_query, w_key, w_value, k_flat, v_flat)
        chunk = jax.ShapeDtypeStruct((per * batch + 8, hd), F32)
        chunk = jax.ShapeDtypeStruct((per * batch + 8, hd), F32)
        k_out, v_out, kring, vring, *chunks = pl.pallas_call(
            functools.partial(attend_kernel, hd ** -0.5),
            out_shape=(cache, cache, ring, ring) + (chunk,) * nseq,
            in_specs=[smem, vmem, any_spec, any_spec, vmem, vmem],
            out_specs=(any_spec, any_spec, vmem, vmem) + (vmem,) * nseq,
            input_output_aliases={4: 2, 5: 3},
            scratch_shapes=[
                pltpu.VMEM((2, batch * heads, 128), F32),
                pltpu.VMEM((batch * heads, 128), F32),
                pltpu.VMEM((batch * heads, 128), F32),
                dma((RING,)), dma((RING,)), dma((RING,)), dma((RING,)),
            ],
            compiler_params=pltpu.CompilerParams(vmem_limit_bytes=4 * 2**20),
        )(positions, qkv, k_flat, v_flat, kring, vring)
        got = [lax.ppermute(chunks[d], "seq", [(i, i ^ d) for i in range(nseq)]) for d in range(1, nseq)]
        k_out, v_out, after = pl.pallas_call(
            write_kernel,
            out_shape=(cache, cache, jax.ShapeDtypeStruct((8, 128), F32)),
            in_specs=[vmem, vmem, any_spec, any_spec, vmem],
            out_specs=(any_spec, any_spec, vmem),
            input_output_aliases={2: 0, 3: 1},
            scratch_shapes=[dma((2 * HELD,))],
            compiler_params=pltpu.CompilerParams(vmem_limit_bytes=1 * 2**20),
            cost_estimate=pl.CostEstimate(flops=10**9, bytes_accessed=8 * HELD * 2**20, transcendentals=0),
        )(kring, vring, k_out, v_out, chunks[0])
        ycols = model // ndev
        y = pl.pallas_call(
            finish_kernel,
            out_shape=jax.ShapeDtypeStruct((batch, model), BF16),
            in_specs=[vmem] * (nseq + 2),
            out_specs=vmem,
            scratch_shapes=[
                pltpu.VMEM((ndev, batch, ycols), F32),
                pltpu.VMEM((ndev, batch, ycols), F32),
                pltpu.VMEM((ndev, batch, ycols), BF16),
                dma((ndev,)), dma((ndev,)), dma((ndev,)), dma((ndev,)),
            ],
            compiler_params=pltpu.CompilerParams(
                collective_id=1, has_side_effects=True, vmem_limit_bytes=6 * 2**20),
        )(chunks[0], *got, w_out, after)
        return y, k_out.reshape(k_cache.shape), v_out.reshape(v_cache.shape)

    return jax.shard_map(
        local_step,
        mesh=mesh,
        in_specs=(P("rep", None), P(), P(), P(), P(("head", "seq"), None), cache_spec, cache_spec, P("rep")),
        out_specs=(P("rep", None), cache_spec, cache_spec),
        check_vma=False,
    )
```

```python
import functools

import jax
import jax.numpy as jnp
from jax import lax
from jax.experimental import pallas as pl
from jax.experimental.pallas import tpu as pltpu
from jax.sharding import PartitionSpec as P

MESH = pl.DeviceIdType.MESH
RING = 8
HELD = 4
AHEAD = 2
PARTS = 4
F32 = jnp.float32
BF16 = jnp.bfloat16
NT = (((1,), (1,)), ((), ()))


def _at(h, s):
    return {"head": h, "seq": s}


def _flip(a, bits):
    for bit in (1, 2, 4):
        if bits & bit:
            a = a + bit * (1 - 2 * lax.rem(a // bit, 2))
    return a


def _greet(peers):
    barrier = pltpu.get_barrier_semaphore()
    for peer in peers:
        pl.semaphore_signal(barrier, inc=1, device_id=peer, device_id_type=MESH)
    return lambda: pl.semaphore_wait(barrier, len(peers))


def project_kernel(x_hbm, wq_ref, wk_ref, wv_ref, k_hbm, v_hbm,
                   qkv_ref, kring, vring,
                   x_ref, wbuf, held, xsem, wsem, ringsem, ssem, rsem):
    nseq = held.shape[0]
    h, s = lax.axis_index("head"), lax.axis_index("seq")
    cols = wbuf.shape[-1]
    rows = wbuf.shape[2]
    first = pl.multiple_of((h * nseq + s) * cols, 128)
    peers = [lax.rem(s + d, nseq) for d in range(1, nseq)]
    joined = _greet([_at(h, p) for p in peers])
    tokens = pltpu.make_async_copy(x_hbm, x_ref, xsem)
    tokens.start()
    loads = []
    for j, w in enumerate((wq_ref, wk_ref, wv_ref)):
        for p in range(PARTS):
            c = pltpu.make_async_copy(
                w.at[pl.ds(p * rows, rows), pl.ds(first, cols)], wbuf.at[j, p], wsem.at[j, p])
            c.start()
            loads.append(c)
    ring = []
    for b in range(HELD):
        for i, (src, dst) in enumerate(((k_hbm, kring), (v_hbm, vring))):
            pair = pl.ds(2 * b, 2)
            ring.append(pltpu.make_async_copy(src.at[pair], dst.at[pair], ringsem.at[i, b]))
    asked = 0
    sends = []
    tokens.wait()
    for j in range(3):
        acc = None
        for p in range(PARTS):
            loads[j * PARTS + p].wait()
            share = -(-len(ring) * (j * PARTS + p + 1) // (3 * PARTS))
            while asked < share:
                ring[asked].start()
                asked += 1
            part = jnp.dot(x_ref[:, p * rows:(p + 1) * rows], wbuf[j, p], preferred_element_type=F32)
            acc = part if acc is None else acc + part
        held[s, j] = acc.astype(BF16)
        if j == 0:
            joined()
        for i, p in enumerate(peers):
            c = pltpu.make_async_remote_copy(
                src_ref=held.at[s, j], dst_ref=held.at[s, j], send_sem=ssem.at[j, i], recv_sem=rsem.at[j, i],
                device_id=_at(h, p), device_id_type=MESH)
            c.start()
            sends.append(c)

    def spread(src, which):
        per = cols // 256
        for j in which:
            for i in range(per):
                for half in range(2):
                    val = held[src, j, :, i * 256 + half * 128:i * 256 + half * 128 + 128].astype(F32)
                    qkv_ref[j, half, pl.ds(src * per + i, val.shape[0], stride=nseq * per), :] = val

    spread(s, range(3))
    for j in range(3):
        for i in range(nseq - 1):
            sends[j * (nseq - 1) + i].wait_recv()
            spread(lax.rem(s + nseq - 1 - i, nseq), (j,))
    for c in sends:
        c.wait_send()
    for c in ring:
        c.wait()


def attend_kernel(scale, pos_ref, qkv_ref, k_hbm, v_hbm, kring_in, vring_in,
                  ko_hbm, vo_hbm, kring, vring, *rest):
    chunks = rest[:-7]
    obuf, mbuf, lbuf, kin, vin, kout, vout = rest[-7:]
    batch, wide, hd = k_hbm.shape
    nseq = len(chunks)
    heads = obuf.shape[1] // batch
    per = heads // nseq
    span = wide // heads
    pairs = batch // 2
    base = lax.axis_index("seq") * span
    col = lax.broadcasted_iota(jnp.int32, (heads, wide), 1)
    row = lax.broadcasted_iota(jnp.int32, (heads, wide), 0)
    own = lax.rem(col, heads) == row
    slot_of = jnp.where(own, base + col // heads, batch * nseq * span)

    def both(i):
        return pl.ds(pl.multiple_of(i * 2, 2), 2)

    flow = RING - HELD

    def place(i):
        return HELD + lax.rem(i - HELD, flow)

    def reads(i):
        slot = place(i)
        return [pltpu.make_async_copy(src.at[both(i)], dst.at[both(slot)], sem.at[slot])
                for src, dst, sem in ((k_hbm, kring, kin), (v_hbm, vring, vin))]

    def writes(i):
        slot = place(i)
        return [pltpu.make_async_copy(src.at[both(slot)], dst.at[both(i)], sem.at[slot])
                for src, dst, sem in ((kring, ko_hbm, kout), (vring, vo_hbm, vout))]

    def fresh(j, lines):
        return jnp.concatenate([qkv_ref[j, 0, lines, :], qkv_ref[j, 1, lines, :]], axis=-1).astype(BF16)

    for i in range(HELD, HELD + flow):
        for c in reads(i):
            c.start()

    def body(i, carry):
        nxt = i + AHEAD

        @pl.when(jnp.logical_and(nxt >= RING, nxt < pairs))
        def _():
            for c in writes(nxt - flow):
                c.wait()
            for c in reads(nxt):
                c.start()

        @pl.when(i >= HELD)
        def _():
            for c in reads(i):
                c.wait()

        rows = []
        for g in range(2):
            b = 2 * i + g
            pos = pos_ref[b]
            at = pos - base
            lines = pl.ds(pl.multiple_of(b * heads, heads), heads)
            spot = pl.ds(pl.multiple_of(at * heads, heads), heads)
            ks = 2 * jnp.where(i < HELD, i, place(jnp.maximum(i, HELD))) + g

            @pl.when(jnp.logical_and(at >= 0, at < span))
            def _():
                kring[ks, spot, :] = fresh(1, lines)
                vring[ks, spot, :] = fresh(2, lines)

            rows.append((b, pos, lines, ks))
        scores = []
        for b, pos, lines, ks in rows:
            score = lax.dot_general(fresh(0, lines), kring[ks], NT, preferred_element_type=F32) * scale
            scores.append(jnp.where(slot_of <= pos, score, -jnp.inf))
        for (b, pos, lines, ks), score in zip(rows, scores):
            top = jnp.max(score, axis=-1, keepdims=True)
            safe = jnp.where(top == -jnp.inf, 0.0, top)
            weight = jnp.exp(score - safe)
            total = jnp.sum(weight, axis=-1, keepdims=True)
            mix = jnp.dot(weight.astype(BF16), vring[ks], preferred_element_type=F32)
            obuf[0, lines, :] = mix[:, :128]
            obuf[1, lines, :] = mix[:, 128:]
            mbuf[lines, :] = jnp.broadcast_to(top, (heads, 128))
            lbuf[lines, :] = jnp.broadcast_to(total, (heads, 128))

        @pl.when(i >= HELD)
        def _():
            for c in writes(i):
                c.start()

        return carry

    lax.fori_loop(0, pairs, body, 0)
    eye = (lax.broadcasted_iota(jnp.int32, (batch, 128), 0)
           == lax.broadcasted_iota(jnp.int32, (batch, 128), 1))
    me = lax.axis_index("seq")
    for d, chunk in enumerate(chunks):
        for e in range(per):
            pick = pl.ds(_flip(me, d) * per + e, batch, stride=heads)
            rows = slice(e * batch, (e + 1) * batch)
            chunk[rows, :128] = obuf[0, pick, :]
            chunk[rows, 128:] = obuf[1, pick, :]
            for i, buf in enumerate((mbuf, lbuf)):
                line = per * batch + 2 * e + i
                chunk[line:line + 1, :128] = jnp.sum(jnp.where(eye, buf[pick, :], 0.0), axis=0, keepdims=True)
                chunk[line:line + 1, 128:] = jnp.zeros((1, hd - 128), F32)
        used = per * batch + 2 * per
        chunk[used:, :] = jnp.zeros((chunk.shape[0] - used, hd), F32)
    for i in range(pairs - flow, pairs):
        for c in writes(i):
            c.wait()


def write_kernel(kring, vring, ko_in, vo_in, chunk, ko_hbm, vo_hbm, done, sem):
    copies = []
    for i in range(HELD):
        for src, dst in ((kring, ko_hbm), (vring, vo_hbm)):
            pair = pl.ds(i * 2, 2)
            c = pltpu.make_async_copy(src.at[pair], dst.at[pair], sem.at[len(copies)])
            c.start()
            copies.append(c)
    done[...] = jnp.zeros_like(done)
    for c in copies:
        c.wait()


def finish_kernel(*refs):
    got = refs[:-14]
    wo, after, y_ref, theirs, ours, half, ygot, yout, s1, r1, s2, r2, s3, r3 = refs[-14:]
    nseq = len(got)
    chips, batch, cols = ours.shape
    ndev = 2 * chips
    hd = got[0].shape[1]
    per = (got[0].shape[0] - 8) // batch
    h, s = lax.axis_index("head"), lax.axis_index("seq")
    me = h * nseq + s
    core, chip = lax.rem(me, 2), me // 2

    def spot(p):
        return _at(p // nseq, lax.rem(p, nseq))

    far = [_flip(me, d) for d in range(ndev - 1, 0, -1)]
    joined = _greet([spot(p) for p in far])
    eye = (lax.broadcasted_iota(jnp.int32, (batch, hd), 0)
           == lax.broadcasted_iota(jnp.int32, (batch, hd), 1))
    attn = []
    for e in range(per):
        line = per * batch + 2 * e
        tops = [got[i][line:line + 1, :] for i in range(nseq)]
        sums = [got[i][line + 1:line + 2, :] for i in range(nseq)]
        top = functools.reduce(jnp.maximum, tops)
        mix, total = None, None
        for i in range(nseq):
            factor = jnp.exp(tops[i] - top)
            share = factor * sums[i]
            total = share if total is None else total + share
            down = jnp.sum(jnp.where(eye, factor, 0.0), axis=1, keepdims=True)
            term = got[i][e * batch:(e + 1) * batch, :] * down
            mix = term if mix is None else mix + term
        down = jnp.sum(jnp.where(eye, total, 0.0), axis=1, keepdims=True)
        attn.append((mix / down).astype(BF16))
    attn = jnp.concatenate(attn, axis=-1)

    def product(j, side):
        at = pl.multiple_of((2 * j + side) * cols, 128)
        return jnp.dot(attn, wo[:, pl.ds(at, cols)], preferred_element_type=F32)

    for j in range(chips):
        theirs[j] = product(j, 1 - core)
    joined()
    swap = pltpu.make_async_remote_copy(
        src_ref=theirs, dst_ref=half, send_sem=s1, recv_sem=r1,
        device_id=spot(_flip(me, 1)), device_id_type=MESH)
    swap.start()
    for j in range(chips):
        ours[j] = product(j, core)
    swap.wait_recv()
    for j in range(chips):
        ours[j] += half[j]
    moves = []
    for i in range(chips - 1):
        there = _flip(chip, chips - 1 - i)
        c = pltpu.make_async_remote_copy(
            src_ref=ours.at[there], dst_ref=ygot.at[i], send_sem=s2.at[i], recv_sem=r2.at[i],
            device_id=spot(2 * there + core), device_id_type=MESH)
        c.start()
        moves.append(c)
    acc = ours[chip]
    for i in range(chips - 2, -1, -1):
        moves[i].wait_recv()
        acc = acc + ygot[i]
    yout[me] = acc.astype(BF16)
    shares = []
    for i, p in enumerate(far):
        c = pltpu.make_async_remote_copy(
            src_ref=yout.at[me], dst_ref=yout.at[me], send_sem=s3.at[i], recv_sem=r3.at[i],
            device_id=spot(p), device_id_type=MESH)
        c.start()
        shares.append(c)
    for c in shares:
        c.wait_recv()
    for p in range(ndev):
        y_ref[:, p * cols:(p + 1) * cols] = yout[p]
    for c in [swap] + moves + shares:
        c.wait_send()


def solution(mesh):
    nhead, nseq = mesh.shape["head"], mesh.shape["seq"]
    ndev = nhead * nseq
    cache_spec = P("rep", "seq", "head", None)
    any_spec = pl.BlockSpec(memory_space=pl.ANY)
    vmem = pl.BlockSpec(memory_space=pltpu.VMEM)
    smem = pl.BlockSpec(memory_space=pltpu.SMEM)

    def local_step(tokens, w_query, w_key, w_value, w_out, k_cache, v_cache, positions):
        batch, span, heads, hd = k_cache.shape
        model = tokens.shape[1]
        cols = heads * hd // nseq
        per = heads // nseq
        cache = jax.ShapeDtypeStruct((batch, span * heads, hd), BF16)
        ring = jax.ShapeDtypeStruct((2 * RING, span * heads, hd), BF16)
        k_flat, v_flat = k_cache.reshape(cache.shape), v_cache.reshape(cache.shape)
        dma = pltpu.SemaphoreType.DMA
        qkv, kring, vring = pl.pallas_call(
            project_kernel,
            out_shape=(jax.ShapeDtypeStruct((3, 2, batch * heads, 128), F32), ring, ring),
            in_specs=[any_spec] * 6,
            out_specs=(vmem, vmem, vmem),
            scratch_shapes=[
                pltpu.VMEM(tokens.shape, BF16),
                pltpu.VMEM((3, PARTS, model // PARTS, cols), BF16),
                pltpu.VMEM((nseq, 3, batch, cols), BF16),
                dma, dma((3, PARTS)), dma((2, HELD)), dma((3, nseq - 1)), dma((3, nseq - 1)),
            ],
            compiler_params=pltpu.CompilerParams(
                collective_id=0, has_side_effects=True, vmem_limit_bytes=11 * 2**20),
        )(pltpu.with_memory_space_constraint(tokens, pltpu.HBM), w_query, w_key, w_value, k_flat, v_flat)
        chunk = jax.ShapeDtypeStruct((per * batch + 8, hd), F32)
        chunk = jax.ShapeDtypeStruct((per * batch + 8, hd), F32)
        k_out, v_out, kring, vring, *chunks = pl.pallas_call(
            functools.partial(attend_kernel, hd ** -0.5),
            out_shape=(cache, cache, ring, ring) + (chunk,) * nseq,
            in_specs=[smem, vmem, any_spec, any_spec, vmem, vmem],
            out_specs=(any_spec, any_spec, vmem, vmem) + (vmem,) * nseq,
            input_output_aliases={4: 2, 5: 3},
            scratch_shapes=[
                pltpu.VMEM((2, batch * heads, 128), F32),
                pltpu.VMEM((batch * heads, 128), F32),
                pltpu.VMEM((batch * heads, 128), F32),
                dma((RING,)), dma((RING,)), dma((RING,)), dma((RING,)),
            ],
            compiler_params=pltpu.CompilerParams(vmem_limit_bytes=4 * 2**20),
        )(positions, qkv, k_flat, v_flat, kring, vring)
        got = [lax.ppermute(chunks[d], "seq", [(i, i ^ d) for i in range(nseq)]) for d in range(1, nseq)]
        k_out, v_out, after = pl.pallas_call(
            write_kernel,
            out_shape=(cache, cache, jax.ShapeDtypeStruct((8, 128), F32)),
            in_specs=[vmem, vmem, any_spec, any_spec, vmem],
            out_specs=(any_spec, any_spec, vmem),
            input_output_aliases={2: 0, 3: 1},
            scratch_shapes=[dma((2 * HELD,))],
            compiler_params=pltpu.CompilerParams(vmem_limit_bytes=1 * 2**20),
            cost_estimate=pl.CostEstimate(flops=10**9, bytes_accessed=8 * HELD * 2**20, transcendentals=0),
        )(kring, vring, k_out, v_out, chunks[0])
        ycols = model // ndev
        y = pl.pallas_call(
            finish_kernel,
            out_shape=jax.ShapeDtypeStruct((batch, model), BF16),
            in_specs=[vmem] * (nseq + 2),
            out_specs=vmem,
            scratch_shapes=[
                pltpu.VMEM((ndev // 2, batch, ycols), F32),
                pltpu.VMEM((ndev // 2, batch, ycols), F32),
                pltpu.VMEM((ndev // 2, batch, ycols), F32),
                pltpu.VMEM((ndev // 2 - 1, batch, ycols), F32),
                pltpu.VMEM((ndev, batch, ycols), BF16),
                dma, dma, dma((ndev // 2 - 1,)), dma((ndev // 2 - 1,)), dma((ndev - 1,)), dma((ndev - 1,)),
            ],
            compiler_params=pltpu.CompilerParams(
                collective_id=1, has_side_effects=True, vmem_limit_bytes=6 * 2**20),
        )(chunks[0], *got, w_out, after)
        return y, k_out.reshape(k_cache.shape), v_out.reshape(v_cache.shape)

    return jax.shard_map(
        local_step,
        mesh=mesh,
        in_specs=(P("rep", None), P(), P(), P(), P(("head", "seq"), None), cache_spec, cache_spec, P("rep")),
        out_specs=(P("rep", None), cache_spec, cache_spec),
        check_vma=False,
    )
```

```python
import functools

import jax
import jax.numpy as jnp
from jax import lax
from jax.experimental import pallas as pl
from jax.experimental.pallas import tpu as pltpu
from jax.sharding import PartitionSpec as P

MESH = pl.DeviceIdType.MESH
RING = 8
HELD = 3
FIRST = 4
AHEAD = 3
LATE = 5
PARTS = 4
F32 = jnp.float32
BF16 = jnp.bfloat16
NT = (((1,), (1,)), ((), ()))


def _at(h, s):
    return {"head": h, "seq": s}


def _flip(a, bits):
    for bit in (1, 2, 4):
        if bits & bit:
            a = a + bit * (1 - 2 * lax.rem(a // bit, 2))
    return a


def _greet(peers):
    barrier = pltpu.get_barrier_semaphore()
    for peer in peers:
        pl.semaphore_signal(barrier, inc=1, device_id=peer, device_id_type=MESH)
    return lambda: pl.semaphore_wait(barrier, len(peers))


def project_kernel(x_hbm, wq_ref, wk_ref, wv_ref, k_hbm, v_hbm,
                   qkv_ref, kring, vring,
                   x_ref, wbuf, held, xsem, wsem, ringsem, ssem, rsem):
    nseq = held.shape[0]
    h, s = lax.axis_index("head"), lax.axis_index("seq")
    cols = wbuf.shape[-1]
    rows = wbuf.shape[2]
    first = pl.multiple_of((h * nseq + s) * cols, 128)
    peers = [lax.rem(s + d, nseq) for d in range(1, nseq)]
    joined = _greet([_at(h, p) for p in peers])
    tokens = pltpu.make_async_copy(x_hbm, x_ref, xsem)
    tokens.start()
    loads = []
    for j, w in enumerate((wq_ref, wk_ref, wv_ref)):
        for p in range(PARTS):
            c = pltpu.make_async_copy(
                w.at[pl.ds(p * rows, rows), pl.ds(first, cols)], wbuf.at[j, p], wsem.at[j, p])
            c.start()
            loads.append(c)
    ring = []
    for b in range(FIRST):
        for i, (src, dst) in enumerate(((k_hbm, kring), (v_hbm, vring))):
            pair = pl.ds(2 * b, 2)
            ring.append(pltpu.make_async_copy(src.at[pair], dst.at[pair], ringsem.at[i, b]))
    asked = 0
    sends = []
    tokens.wait()
    for j in range(3):
        acc = None
        for p in range(PARTS):
            loads[j * PARTS + p].wait()
            share = len(ring) * (j * PARTS + p + 1 - LATE) // (3 * PARTS - LATE)
            while asked < share:
                ring[asked].start()
                asked += 1
            part = jnp.dot(x_ref[:, p * rows:(p + 1) * rows], wbuf[j, p], preferred_element_type=F32)
            acc = part if acc is None else acc + part
        held[s, j] = acc.astype(BF16)
        if j == 0:
            joined()
        for i, p in enumerate(peers):
            c = pltpu.make_async_remote_copy(
                src_ref=held.at[s, j], dst_ref=held.at[s, j], send_sem=ssem.at[j, i], recv_sem=rsem.at[j, i],
                device_id=_at(h, p), device_id_type=MESH)
            c.start()
            sends.append(c)

    def spread(src, which):
        per = cols // 256
        for j in which:
            for i in range(per):
                for half in range(2):
                    val = held[src, j, :, i * 256 + half * 128:i * 256 + half * 128 + 128].astype(F32)
                    qkv_ref[j, half, pl.ds(src * per + i, val.shape[0], stride=nseq * per), :] = val

    spread(s, range(3))
    for j in range(3):
        for i in range(nseq - 1):
            sends[j * (nseq - 1) + i].wait_recv()
            spread(lax.rem(s + nseq - 1 - i, nseq), (j,))
    for c in sends:
        c.wait_send()
    for c in ring:
        c.wait()


def attend_kernel(scale, pos_ref, qkv_ref, k_hbm, v_hbm, kring_in, vring_in,
                  ko_hbm, vo_hbm, kring, vring, *rest):
    chunks = rest[:-7]
    obuf, mbuf, lbuf, kin, vin, kout, vout = rest[-7:]
    batch, wide, hd = k_hbm.shape
    nseq = len(chunks)
    heads = obuf.shape[1] // batch
    per = heads // nseq
    span = wide // heads
    pairs = batch // 2
    base = lax.axis_index("seq") * span
    col = lax.broadcasted_iota(jnp.int32, (heads, wide), 1)
    row = lax.broadcasted_iota(jnp.int32, (heads, wide), 0)
    own = lax.rem(col, heads) == row
    slot_of = jnp.where(own, base + col // heads, batch * nseq * span)

    def both(i):
        return pl.ds(pl.multiple_of(i * 2, 2), 2)

    flow = RING - HELD

    def place(i):
        return HELD + lax.rem(i - HELD, flow)

    def reads(i):
        slot = place(i)
        return [pltpu.make_async_copy(src.at[both(i)], dst.at[both(slot)], sem.at[slot])
                for src, dst, sem in ((k_hbm, kring, kin), (v_hbm, vring, vin))]

    def writes(i):
        slot = place(i)
        return [pltpu.make_async_copy(src.at[both(slot)], dst.at[both(i)], sem.at[slot])
                for src, dst, sem in ((kring, ko_hbm, kout), (vring, vo_hbm, vout))]

    def fresh(j, lines):
        return jnp.concatenate([qkv_ref[j, 0, lines, :], qkv_ref[j, 1, lines, :]], axis=-1).astype(BF16)

    for i in range(FIRST, FIRST + 2):
        for c in reads(i):
            c.start()

    def body(i, carry):
        nxt = i + AHEAD

        @pl.when(jnp.logical_and(nxt >= FIRST + 2, nxt < pairs))
        def _():
            @pl.when(nxt >= RING)
            def _():
                for c in writes(nxt - flow):
                    c.wait()

            for c in reads(nxt):
                c.start()

        @pl.when(i >= FIRST)
        def _():
            for c in reads(i):
                c.wait()

        rows = []
        for g in range(2):
            b = 2 * i + g
            pos = pos_ref[b]
            at = pos - base
            lines = pl.ds(pl.multiple_of(b * heads, heads), heads)
            spot = pl.ds(pl.multiple_of(at * heads, heads), heads)
            ks = 2 * jnp.where(i < HELD, i, place(jnp.maximum(i, HELD))) + g

            @pl.when(jnp.logical_and(at >= 0, at < span))
            def _():
                kring[ks, spot, :] = fresh(1, lines)
                vring[ks, spot, :] = fresh(2, lines)

            rows.append((b, pos, lines, ks))
        scores = []
        for b, pos, lines, ks in rows:
            score = lax.dot_general(fresh(0, lines), kring[ks], NT, preferred_element_type=F32) * scale
            scores.append(jnp.where(slot_of <= pos, score, -jnp.inf))
        for (b, pos, lines, ks), score in zip(rows, scores):
            top = jnp.max(score, axis=-1, keepdims=True)
            safe = jnp.where(top == -jnp.inf, 0.0, top)
            weight = jnp.exp(score - safe)
            total = jnp.sum(weight, axis=-1, keepdims=True)
            mix = jnp.dot(weight.astype(BF16), vring[ks], preferred_element_type=F32)
            obuf[0, lines, :] = mix[:, :128]
            obuf[1, lines, :] = mix[:, 128:]
            mbuf[lines, :] = jnp.broadcast_to(top, (heads, 128))
            lbuf[lines, :] = jnp.broadcast_to(total, (heads, 128))

        @pl.when(jnp.logical_and(i >= HELD, i < pairs - 1))
        def _():
            for c in writes(i):
                c.start()

        return carry

    lax.fori_loop(0, pairs, body, 0)
    eye = (lax.broadcasted_iota(jnp.int32, (batch, 128), 0)
           == lax.broadcasted_iota(jnp.int32, (batch, 128), 1))
    me = lax.axis_index("seq")
    for d, chunk in enumerate(chunks):
        for e in range(per):
            pick = pl.ds(_flip(me, d) * per + e, batch, stride=heads)
            rows = slice(e * batch, (e + 1) * batch)
            chunk[rows, :128] = obuf[0, pick, :]
            chunk[rows, 128:] = obuf[1, pick, :]
            for i, buf in enumerate((mbuf, lbuf)):
                line = per * batch + 2 * e + i
                chunk[line:line + 1, :128] = jnp.sum(jnp.where(eye, buf[pick, :], 0.0), axis=0, keepdims=True)
                chunk[line:line + 1, 128:] = jnp.zeros((1, hd - 128), F32)
        used = per * batch + 2 * per
        chunk[used:, :] = jnp.zeros((chunk.shape[0] - used, hd), F32)
    for i in range(pairs - flow, pairs - 1):
        for c in writes(i):
            c.wait()


def write_kernel(kring, vring, ko_in, vo_in, chunk, ko_hbm, vo_hbm, done, sem):
    pairs = ko_hbm.shape[0] // 2
    last = HELD + (pairs - 1 - HELD) % (RING - HELD)
    copies = []
    for i, slot in [(i, i) for i in range(HELD)] + [(pairs - 1, last)]:
        for src, dst in ((kring, ko_hbm), (vring, vo_hbm)):
            c = pltpu.make_async_copy(
                src.at[pl.ds(slot * 2, 2)], dst.at[pl.ds(i * 2, 2)], sem.at[len(copies)])
            c.start()
            copies.append(c)
    done[...] = jnp.zeros_like(done)
    for c in copies:
        c.wait()


def finish_kernel(*refs):
    got = refs[:-14]
    wo, after, y_ref, theirs, ours, half, ygot, yout, s1, r1, s2, r2, s3, r3 = refs[-14:]
    nseq = len(got)
    chips, batch, cols = ours.shape
    ndev = 2 * chips
    hd = got[0].shape[1]
    per = (got[0].shape[0] - 8) // batch
    h, s = lax.axis_index("head"), lax.axis_index("seq")
    me = h * nseq + s
    core, chip = lax.rem(me, 2), me // 2

    def spot(p):
        return _at(p // nseq, lax.rem(p, nseq))

    far = [_flip(me, d) for d in range(ndev - 1, 0, -1)]
    joined = _greet([spot(p) for p in far])
    eye = (lax.broadcasted_iota(jnp.int32, (batch, hd), 0)
           == lax.broadcasted_iota(jnp.int32, (batch, hd), 1))
    attn = []
    for e in range(per):
        line = per * batch + 2 * e
        tops = [got[i][line:line + 1, :] for i in range(nseq)]
        sums = [got[i][line + 1:line + 2, :] for i in range(nseq)]
        top = functools.reduce(jnp.maximum, tops)
        mix, total = None, None
        for i in range(nseq):
            factor = jnp.exp(tops[i] - top)
            share = factor * sums[i]
            total = share if total is None else total + share
            down = jnp.sum(jnp.where(eye, factor, 0.0), axis=1, keepdims=True)
            term = got[i][e * batch:(e + 1) * batch, :] * down
            mix = term if mix is None else mix + term
        down = jnp.sum(jnp.where(eye, total, 0.0), axis=1, keepdims=True)
        attn.append((mix / down).astype(BF16))
    attn = jnp.concatenate(attn, axis=-1)

    def product(j, side):
        at = pl.multiple_of((2 * j + side) * cols, 128)
        return jnp.dot(attn, wo[:, pl.ds(at, cols)], preferred_element_type=F32)

    for j in range(chips):
        theirs[j] = product(j, 1 - core)
    joined()
    swap = pltpu.make_async_remote_copy(
        src_ref=theirs, dst_ref=half, send_sem=s1, recv_sem=r1,
        device_id=spot(_flip(me, 1)), device_id_type=MESH)
    swap.start()
    for j in range(chips):
        ours[j] = product(j, core)
    swap.wait_recv()
    for j in range(chips):
        ours[j] += half[j]
    moves = []
    for i in range(chips - 1):
        there = _flip(chip, chips - 1 - i)
        c = pltpu.make_async_remote_copy(
            src_ref=ours.at[there], dst_ref=ygot.at[i], send_sem=s2.at[i], recv_sem=r2.at[i],
            device_id=spot(2 * there + core), device_id_type=MESH)
        c.start()
        moves.append(c)
    acc = ours[chip]
    for i in range(chips - 2, -1, -1):
        moves[i].wait_recv()
        acc = acc + ygot[i]
    yout[me] = acc.astype(BF16)
    shares = []
    for i, p in enumerate(far):
        c = pltpu.make_async_remote_copy(
            src_ref=yout.at[me], dst_ref=yout.at[me], send_sem=s3.at[i], recv_sem=r3.at[i],
            device_id=spot(p), device_id_type=MESH)
        c.start()
        shares.append(c)
    for c in shares:
        c.wait_recv()
    for p in range(ndev):
        y_ref[:, p * cols:(p + 1) * cols] = yout[p]
    for c in [swap] + moves + shares:
        c.wait_send()


def solution(mesh):
    nhead, nseq = mesh.shape["head"], mesh.shape["seq"]
    ndev = nhead * nseq
    cache_spec = P("rep", "seq", "head", None)
    any_spec = pl.BlockSpec(memory_space=pl.ANY)
    vmem = pl.BlockSpec(memory_space=pltpu.VMEM)
    smem = pl.BlockSpec(memory_space=pltpu.SMEM)

    def local_step(tokens, w_query, w_key, w_value, w_out, k_cache, v_cache, positions):
        batch, span, heads, hd = k_cache.shape
        model = tokens.shape[1]
        cols = heads * hd // nseq
        per = heads // nseq
        cache = jax.ShapeDtypeStruct((batch, span * heads, hd), BF16)
        ring = jax.ShapeDtypeStruct((2 * RING, span * heads, hd), BF16)
        k_flat, v_flat = k_cache.reshape(cache.shape), v_cache.reshape(cache.shape)
        dma = pltpu.SemaphoreType.DMA
        qkv, kring, vring = pl.pallas_call(
            project_kernel,
            out_shape=(jax.ShapeDtypeStruct((3, 2, batch * heads, 128), F32), ring, ring),
            in_specs=[any_spec] * 6,
            out_specs=(vmem, vmem, vmem),
            scratch_shapes=[
                pltpu.VMEM(tokens.shape, BF16),
                pltpu.VMEM((3, PARTS, model // PARTS, cols), BF16),
                pltpu.VMEM((nseq, 3, batch, cols), BF16),
                dma, dma((3, PARTS)), dma((2, FIRST)), dma((3, nseq - 1)), dma((3, nseq - 1)),
            ],
            compiler_params=pltpu.CompilerParams(
                collective_id=0, has_side_effects=True, vmem_limit_bytes=11 * 2**20),
        )(pltpu.with_memory_space_constraint(tokens, pltpu.HBM), w_query, w_key, w_value, k_flat, v_flat)
        chunk = jax.ShapeDtypeStruct((per * batch + 8, hd), F32)
        chunk = jax.ShapeDtypeStruct((per * batch + 8, hd), F32)
        k_out, v_out, kring, vring, *chunks = pl.pallas_call(
            functools.partial(attend_kernel, hd ** -0.5),
            out_shape=(cache, cache, ring, ring) + (chunk,) * nseq,
            in_specs=[smem, vmem, any_spec, any_spec, vmem, vmem],
            out_specs=(any_spec, any_spec, vmem, vmem) + (vmem,) * nseq,
            input_output_aliases={4: 2, 5: 3},
            scratch_shapes=[
                pltpu.VMEM((2, batch * heads, 128), F32),
                pltpu.VMEM((batch * heads, 128), F32),
                pltpu.VMEM((batch * heads, 128), F32),
                dma((RING,)), dma((RING,)), dma((RING,)), dma((RING,)),
            ],
            compiler_params=pltpu.CompilerParams(vmem_limit_bytes=4 * 2**20),
        )(positions, qkv, k_flat, v_flat, kring, vring)
        got = [lax.ppermute(chunks[d], "seq", [(i, i ^ d) for i in range(nseq)]) for d in range(1, nseq)]
        k_out, v_out, after = pl.pallas_call(
            write_kernel,
            out_shape=(cache, cache, jax.ShapeDtypeStruct((8, 128), F32)),
            in_specs=[vmem, vmem, any_spec, any_spec, vmem],
            out_specs=(any_spec, any_spec, vmem),
            input_output_aliases={2: 0, 3: 1},
            scratch_shapes=[dma((2 * HELD + 2,))],
            compiler_params=pltpu.CompilerParams(vmem_limit_bytes=1 * 2**20),
            cost_estimate=pl.CostEstimate(flops=10**9, bytes_accessed=2**24, transcendentals=0),
        )(kring, vring, k_out, v_out, chunks[0])
        ycols = model // ndev
        y = pl.pallas_call(
            finish_kernel,
            out_shape=jax.ShapeDtypeStruct((batch, model), BF16),
            in_specs=[vmem] * (nseq + 2),
            out_specs=vmem,
            scratch_shapes=[
                pltpu.VMEM((ndev // 2, batch, ycols), F32),
                pltpu.VMEM((ndev // 2, batch, ycols), F32),
                pltpu.VMEM((ndev // 2, batch, ycols), F32),
                pltpu.VMEM((ndev // 2 - 1, batch, ycols), F32),
                pltpu.VMEM((ndev, batch, ycols), BF16),
                dma, dma, dma((ndev // 2 - 1,)), dma((ndev // 2 - 1,)), dma((ndev - 1,)), dma((ndev - 1,)),
            ],
            compiler_params=pltpu.CompilerParams(
                collective_id=1, has_side_effects=True, vmem_limit_bytes=6 * 2**20),
        )(chunks[0], *got, w_out, after)
        return y, k_out.reshape(k_cache.shape), v_out.reshape(v_cache.shape)

    return jax.shard_map(
        local_step,
        mesh=mesh,
        in_specs=(P("rep", None), P(), P(), P(), P(("head", "seq"), None), cache_spec, cache_spec, P("rep")),
        out_specs=(P("rep", None), cache_spec, cache_spec),
        check_vma=False,
    )
```

```python
import functools

import jax
import jax.numpy as jnp
from jax import lax
from jax.experimental import pallas as pl
from jax.experimental.pallas import tpu as pltpu
from jax.sharding import PartitionSpec as P

MESH = pl.DeviceIdType.MESH
BURST = 4
RING = 2 * BURST
FIRST = 4
EARLY = 3
PARTS = 1
F32 = jnp.float32
BF16 = jnp.bfloat16
NT = (((1,), (1,)), ((), ()))


def _at(h, s):
    return {"head": h, "seq": s}


def _flip(a, bits):
    for bit in (1, 2, 4):
        if bits & bit:
            a = a + bit * (1 - 2 * lax.rem(a // bit, 2))
    return a


def _greet(peers):
    barrier = pltpu.get_barrier_semaphore()
    for peer in peers:
        pl.semaphore_signal(barrier, inc=1, device_id=peer, device_id_type=MESH)
    return lambda: pl.semaphore_wait(barrier, len(peers))


def project_kernel(x_hbm, wq_ref, wk_ref, wv_ref, k_hbm, v_hbm,
                   qkv_ref, kring, vring,
                   x_ref, wbuf, held, xsem, wsem, ringsem, ssem, rsem):
    nseq = held.shape[0]
    h, s = lax.axis_index("head"), lax.axis_index("seq")
    cols = wbuf.shape[-1]
    rows = wbuf.shape[2]
    first = pl.multiple_of((h * nseq + s) * cols, 128)
    peers = [lax.rem(s + d, nseq) for d in range(1, nseq)]
    joined = _greet([_at(h, p) for p in peers])
    tokens = pltpu.make_async_copy(x_hbm, x_ref, xsem)
    tokens.start()
    loads = []
    for j, w in enumerate((wq_ref, wk_ref, wv_ref)):
        for p in range(PARTS):
            c = pltpu.make_async_copy(
                w.at[pl.ds(p * rows, rows), pl.ds(first, cols)], wbuf.at[j, p], wsem.at[j, p])
            c.start()
            loads.append(c)
    ring = []
    for b in range(FIRST):
        for i, (src, dst) in enumerate(((k_hbm, kring), (v_hbm, vring))):
            pair = pl.ds(2 * b, 2)
            ring.append(pltpu.make_async_copy(src.at[pair], dst.at[pair], ringsem.at[i, b]))
    asked = 0
    sends = []
    tokens.wait()
    for j in range(3):
        acc = None
        for p in range(PARTS):
            loads[j * PARTS + p].wait()
            share = -(-len(ring) * (j * PARTS + p + 1) // (3 * PARTS))
            while asked < share:
                ring[asked].start()
                asked += 1
            part = jnp.dot(x_ref[:, p * rows:(p + 1) * rows], wbuf[j, p], preferred_element_type=F32)
            acc = part if acc is None else acc + part
        held[s, j] = acc.astype(BF16)
        if j == 0:
            joined()
        for i, p in enumerate(peers):
            c = pltpu.make_async_remote_copy(
                src_ref=held.at[s, j], dst_ref=held.at[s, j], send_sem=ssem.at[j, i], recv_sem=rsem.at[j, i],
                device_id=_at(h, p), device_id_type=MESH)
            c.start()
            sends.append(c)

    def spread(src, which):
        per = cols // 256
        for j in which:
            for i in range(per):
                for half in range(2):
                    val = held[src, j, :, i * 256 + half * 128:i * 256 + half * 128 + 128].astype(F32)
                    qkv_ref[j, half, pl.ds(src * per + i, val.shape[0], stride=nseq * per), :] = val

    spread(s, range(3))
    for j in range(3):
        for i in range(nseq - 1):
            sends[j * (nseq - 1) + i].wait_recv()
            spread(lax.rem(s + nseq - 1 - i, nseq), (j,))
    for c in sends:
        c.wait_send()
    for c in ring:
        c.wait()


def attend_kernel(scale, pos_ref, qkv_ref, k_hbm, v_hbm, kring_in, vring_in,
                  ko_hbm, vo_hbm, kring, vring, *rest):
    chunks = rest[:-7]
    obuf, mbuf, lbuf, kin, vin, kout, vout = rest[-7:]
    batch, wide, hd = k_hbm.shape
    nseq = len(chunks)
    heads = obuf.shape[1] // batch
    per = heads // nseq
    span = wide // heads
    pairs = batch // 2
    base = lax.axis_index("seq") * span
    col = lax.broadcasted_iota(jnp.int32, (heads, wide), 1)
    row = lax.broadcasted_iota(jnp.int32, (heads, wide), 0)
    own = lax.rem(col, heads) == row
    slot_of = jnp.where(own, base + col // heads, batch * nseq * span)

    def both(i):
        return pl.ds(pl.multiple_of(i * 2, 2), 2)

    def reads(i):
        slot = lax.rem(i, RING)
        return [pltpu.make_async_copy(src.at[both(i)], dst.at[both(slot)], sem.at[slot])
                for src, dst, sem in ((k_hbm, kring, kin), (v_hbm, vring, vin))]

    def writes(i):
        slot = lax.rem(i, RING)
        return [pltpu.make_async_copy(src.at[2 * slot + g], dst.at[2 * i + g], sem.at[2 * slot + g])
                for g in range(2) for src, dst, sem in ((kring, ko_hbm, kout), (vring, vo_hbm, vout))]

    def fresh(j, lines):
        return jnp.concatenate([qkv_ref[j, 0, lines, :], qkv_ref[j, 1, lines, :]], axis=-1).astype(BF16)

    for i in range(FIRST, RING):
        for c in reads(i):
            c.start()

    def body(i, carry):
        step = lax.rem(i, BURST)
        slot = lax.rem(i, RING)

        @pl.when(jnp.logical_and(step == 0, i > 0))
        def _():
            for g in range(EARLY):
                if g < FIRST - BURST:
                    @pl.when(i > BURST)
                    def _():
                        for c in reads(i + g):
                            c.wait()
                else:
                    for c in reads(i + g):
                        c.wait()
            for g in range(BURST):
                for c in writes(i - BURST + g):
                    c.start()

        @pl.when(jnp.logical_and(step >= EARLY, i >= FIRST))
        def _():
            for c in reads(i):
                c.wait()

        rows = []
        for g in range(2):
            b = 2 * i + g
            pos = pos_ref[b]
            at = pos - base
            lines = pl.ds(pl.multiple_of(b * heads, heads), heads)
            spot = pl.ds(pl.multiple_of(at * heads, heads), heads)
            ks = 2 * slot + g

            @pl.when(jnp.logical_and(at >= 0, at < span))
            def _():
                kring[ks, spot, :] = fresh(1, lines)
                vring[ks, spot, :] = fresh(2, lines)

            rows.append((b, pos, lines, ks))
        scores = []
        for b, pos, lines, ks in rows:
            score = lax.dot_general(fresh(0, lines), kring[ks], NT, preferred_element_type=F32) * scale
            scores.append(jnp.where(slot_of <= pos, score, -jnp.inf))
        for (b, pos, lines, ks), score in zip(rows, scores):
            top = jnp.max(score, axis=-1, keepdims=True)
            safe = jnp.where(top == -jnp.inf, 0.0, top)
            weight = jnp.exp(score - safe)
            total = jnp.sum(weight, axis=-1, keepdims=True)
            mix = jnp.dot(weight.astype(BF16), vring[ks], preferred_element_type=F32)
            obuf[0, lines, :] = mix[:, :128]
            obuf[1, lines, :] = mix[:, 128:]
            mbuf[lines, :] = jnp.broadcast_to(top, (heads, 128))
            lbuf[lines, :] = jnp.broadcast_to(total, (heads, 128))

        @pl.when(jnp.logical_and(step == BURST - 1, jnp.logical_and(i > BURST, i < pairs - 1)))
        def _():
            for g in range(BURST):
                for c in writes(i + 1 - 2 * BURST + g):
                    c.wait()
                for c in reads(i + 1 + g):
                    c.start()

        return carry

    lax.fori_loop(0, pairs, body, 0)
    eye = (lax.broadcasted_iota(jnp.int32, (batch, 128), 0)
           == lax.broadcasted_iota(jnp.int32, (batch, 128), 1))
    me = lax.axis_index("seq")
    for d, chunk in enumerate(chunks):
        for e in range(per):
            pick = pl.ds(_flip(me, d) * per + e, batch, stride=heads)
            rows = slice(e * batch, (e + 1) * batch)
            chunk[rows, :128] = obuf[0, pick, :]
            chunk[rows, 128:] = obuf[1, pick, :]
            for i, buf in enumerate((mbuf, lbuf)):
                line = per * batch + 2 * e + i
                chunk[line:line + 1, :128] = jnp.sum(jnp.where(eye, buf[pick, :], 0.0), axis=0, keepdims=True)
                chunk[line:line + 1, 128:] = jnp.zeros((1, hd - 128), F32)
        used = per * batch + 2 * per
        chunk[used:, :] = jnp.zeros((chunk.shape[0] - used, hd), F32)
    for i in range(pairs - 2 * BURST, pairs - BURST):
        for c in writes(i):
            c.wait()


def write_kernel(kring, vring, ko_in, vo_in, chunk, ko_hbm, vo_hbm, done, sem):
    pairs = ko_hbm.shape[0] // 2
    copies = []
    for i in range(pairs - BURST, pairs):
        for src, dst in ((kring, ko_hbm), (vring, vo_hbm)):
            c = pltpu.make_async_copy(
                src.at[pl.ds(i % RING * 2, 2)], dst.at[pl.ds(i * 2, 2)], sem.at[len(copies)])
            c.start()
            copies.append(c)
    done[...] = jnp.zeros_like(done)
    for c in copies:
        c.wait()


def finish_kernel(*refs):
    got = refs[:-14]
    wo, after, y_ref, theirs, ours, half, ygot, yout, s1, r1, s2, r2, s3, r3 = refs[-14:]
    nseq = len(got)
    chips, batch, cols = ours.shape
    ndev = 2 * chips
    hd = got[0].shape[1]
    per = (got[0].shape[0] - 8) // batch
    h, s = lax.axis_index("head"), lax.axis_index("seq")
    me = h * nseq + s
    core, chip = lax.rem(me, 2), me // 2

    def spot(p):
        return _at(p // nseq, lax.rem(p, nseq))

    far = [_flip(me, d) for d in range(ndev - 1, 0, -1)]
    joined = _greet([spot(p) for p in far])
    eye = (lax.broadcasted_iota(jnp.int32, (batch, hd), 0)
           == lax.broadcasted_iota(jnp.int32, (batch, hd), 1))
    attn = []
    for e in range(per):
        line = per * batch + 2 * e
        tops = [got[i][line:line + 1, :] for i in range(nseq)]
        sums = [got[i][line + 1:line + 2, :] for i in range(nseq)]
        top = functools.reduce(jnp.maximum, tops)
        mix, total = None, None
        for i in range(nseq):
            factor = jnp.exp(tops[i] - top)
            share = factor * sums[i]
            total = share if total is None else total + share
            down = jnp.sum(jnp.where(eye, factor, 0.0), axis=1, keepdims=True)
            term = got[i][e * batch:(e + 1) * batch, :] * down
            mix = term if mix is None else mix + term
        down = jnp.sum(jnp.where(eye, total, 0.0), axis=1, keepdims=True)
        attn.append((mix / down).astype(BF16))
    attn = jnp.concatenate(attn, axis=-1)

    def product(j, side):
        at = pl.multiple_of((2 * j + side) * cols, 128)
        return jnp.dot(attn, wo[:, pl.ds(at, cols)], preferred_element_type=F32)

    for j in range(chips):
        theirs[j] = product(j, 1 - core)
    joined()
    swap = pltpu.make_async_remote_copy(
        src_ref=theirs, dst_ref=half, send_sem=s1, recv_sem=r1,
        device_id=spot(_flip(me, 1)), device_id_type=MESH)
    swap.start()
    for j in range(chips):
        ours[j] = product(j, core)
    swap.wait_recv()
    for j in range(chips):
        ours[j] += half[j]
    moves = []
    for i in range(chips - 1):
        there = _flip(chip, chips - 1 - i)
        c = pltpu.make_async_remote_copy(
            src_ref=ours.at[there], dst_ref=ygot.at[i], send_sem=s2.at[i], recv_sem=r2.at[i],
            device_id=spot(2 * there + core), device_id_type=MESH)
        c.start()
        moves.append(c)
    acc = ours[chip]
    for i in range(chips - 2, -1, -1):
        moves[i].wait_recv()
        acc = acc + ygot[i]
    yout[me] = acc.astype(BF16)
    shares = []
    for i, p in enumerate(far):
        c = pltpu.make_async_remote_copy(
            src_ref=yout.at[me], dst_ref=yout.at[me], send_sem=s3.at[i], recv_sem=r3.at[i],
            device_id=spot(p), device_id_type=MESH)
        c.start()
        shares.append(c)
    for c in shares:
        c.wait_recv()
    for p in range(ndev):
        y_ref[:, p * cols:(p + 1) * cols] = yout[p]
    for c in [swap] + moves + shares:
        c.wait_send()


def solution(mesh):
    nhead, nseq = mesh.shape["head"], mesh.shape["seq"]
    ndev = nhead * nseq
    cache_spec = P("rep", "seq", "head", None)
    any_spec = pl.BlockSpec(memory_space=pl.ANY)
    vmem = pl.BlockSpec(memory_space=pltpu.VMEM)
    smem = pl.BlockSpec(memory_space=pltpu.SMEM)

    def local_step(tokens, w_query, w_key, w_value, w_out, k_cache, v_cache, positions):
        batch, span, heads, hd = k_cache.shape
        model = tokens.shape[1]
        cols = heads * hd // nseq
        per = heads // nseq
        cache = jax.ShapeDtypeStruct((batch, span * heads, hd), BF16)
        ring = jax.ShapeDtypeStruct((2 * RING, span * heads, hd), BF16)
        k_flat, v_flat = k_cache.reshape(cache.shape), v_cache.reshape(cache.shape)
        dma = pltpu.SemaphoreType.DMA
        qkv, kring, vring = pl.pallas_call(
            project_kernel,
            out_shape=(jax.ShapeDtypeStruct((3, 2, batch * heads, 128), F32), ring, ring),
            in_specs=[any_spec] * 6,
            out_specs=(vmem, vmem, vmem),
            scratch_shapes=[
                pltpu.VMEM(tokens.shape, BF16),
                pltpu.VMEM((3, PARTS, model // PARTS, cols), BF16),
                pltpu.VMEM((nseq, 3, batch, cols), BF16),
                dma, dma((3, PARTS)), dma((2, FIRST)), dma((3, nseq - 1)), dma((3, nseq - 1)),
            ],
            compiler_params=pltpu.CompilerParams(
                collective_id=0, has_side_effects=True, vmem_limit_bytes=11 * 2**20),
        )(pltpu.with_memory_space_constraint(tokens, pltpu.HBM), w_query, w_key, w_value, k_flat, v_flat)
        chunk = jax.ShapeDtypeStruct((per * batch + 8, hd), F32)
        chunk = jax.ShapeDtypeStruct((per * batch + 8, hd), F32)
        k_out, v_out, kring, vring, *chunks = pl.pallas_call(
            functools.partial(attend_kernel, hd ** -0.5),
            out_shape=(cache, cache, ring, ring) + (chunk,) * nseq,
            in_specs=[smem, vmem, any_spec, any_spec, vmem, vmem],
            out_specs=(any_spec, any_spec, vmem, vmem) + (vmem,) * nseq,
            input_output_aliases={4: 2, 5: 3},
            scratch_shapes=[
                pltpu.VMEM((2, batch * heads, 128), F32),
                pltpu.VMEM((batch * heads, 128), F32),
                pltpu.VMEM((batch * heads, 128), F32),
                dma((2 * RING,)), dma((2 * RING,)), dma((2 * RING,)), dma((2 * RING,)),
            ],
            compiler_params=pltpu.CompilerParams(vmem_limit_bytes=4 * 2**20),
        )(positions, qkv, k_flat, v_flat, kring, vring)
        got = [lax.ppermute(chunks[d], "seq", [(i, i ^ d) for i in range(nseq)]) for d in range(1, nseq)]
        k_out, v_out, after = pl.pallas_call(
            write_kernel,
            out_shape=(cache, cache, jax.ShapeDtypeStruct((8, 128), F32)),
            in_specs=[vmem, vmem, any_spec, any_spec, vmem],
            out_specs=(any_spec, any_spec, vmem),
            input_output_aliases={2: 0, 3: 1},
            scratch_shapes=[dma((2 * BURST,))],
            compiler_params=pltpu.CompilerParams(vmem_limit_bytes=1 * 2**20),
            cost_estimate=pl.CostEstimate(flops=10**9, bytes_accessed=2**24, transcendentals=0),
        )(kring, vring, k_out, v_out, chunks[0])
        ycols = model // ndev
        y = pl.pallas_call(
            finish_kernel,
            out_shape=jax.ShapeDtypeStruct((batch, model), BF16),
            in_specs=[vmem] * (nseq + 2),
            out_specs=vmem,
            scratch_shapes=[
                pltpu.VMEM((ndev // 2, batch, ycols), F32),
                pltpu.VMEM((ndev // 2, batch, ycols), F32),
                pltpu.VMEM((ndev // 2, batch, ycols), F32),
                pltpu.VMEM((ndev // 2 - 1, batch, ycols), F32),
                pltpu.VMEM((ndev, batch, ycols), BF16),
                dma, dma, dma((ndev // 2 - 1,)), dma((ndev // 2 - 1,)), dma((ndev - 1,)), dma((ndev - 1,)),
            ],
            compiler_params=pltpu.CompilerParams(
                collective_id=1, has_side_effects=True, vmem_limit_bytes=6 * 2**20),
        )(chunks[0], *got, w_out, after)
        return y, k_out.reshape(k_cache.shape), v_out.reshape(v_cache.shape)

    return jax.shard_map(
        local_step,
        mesh=mesh,
        in_specs=(P("rep", None), P(), P(), P(), P(("head", "seq"), None), cache_spec, cache_spec, P("rep")),
        out_specs=(P("rep", None), cache_spec, cache_spec),
        check_vma=False,
    )
```

```python
import functools

import jax
import jax.numpy as jnp
from jax import lax
from jax.experimental import pallas as pl
from jax.experimental.pallas import tpu as pltpu
from jax.sharding import PartitionSpec as P

MESH = pl.DeviceIdType.MESH
RING = 8
MORE = 2
FIRST = 4
KEPT = 4
SLOTS = (0, 1, 2, 3, 4, 5, 6, 7, 8, 9, 0, 1, 2, 3, 4, 5)


def _plan(text):
    return [(step[0], int(step[1:])) for step in text.split()]


PLAN = (
    _plan("r4 r5 r6 r7 a0 a1 a2 a3")
    + _plan("R4 R5 R6 w0 w1 w2 w3")
    + _plan("a4 a5 a6 R7 a7 r8 r9")
    + _plan("W0 r10 W1 r11 W2 r12 W3 r13")
    + _plan("R8 a8 R9 a9 R10 R11 R12")
    + _plan("w4 w5 w6 w7 a10 w8 w9 a11")
    + _plan("W4 r14 W5 r15 w10 w11 a12")
    + _plan("R13 a13 R14 a14 R15 a15")
    + _plan("W6 W7 W8 W9 W10 W11")
)
PARTS = 1
F32 = jnp.float32
BF16 = jnp.bfloat16
NT = (((1,), (1,)), ((), ()))


def _at(h, s):
    return {"head": h, "seq": s}


def _flip(a, bits):
    for bit in (1, 2, 4):
        if bits & bit:
            a = a + bit * (1 - 2 * lax.rem(a // bit, 2))
    return a


def _greet(peers):
    barrier = pltpu.get_barrier_semaphore()
    for peer in peers:
        pl.semaphore_signal(barrier, inc=1, device_id=peer, device_id_type=MESH)
    return lambda: pl.semaphore_wait(barrier, len(peers))


def project_kernel(x_hbm, wq_ref, wk_ref, wv_ref, k_hbm, v_hbm,
                   qkv_ref, kring, vring,
                   x_ref, wbuf, held, xsem, wsem, ringsem, ssem, rsem):
    nseq = held.shape[0]
    h, s = lax.axis_index("head"), lax.axis_index("seq")
    cols = wbuf.shape[-1]
    rows = wbuf.shape[2]
    first = pl.multiple_of((h * nseq + s) * cols, 128)
    peers = [lax.rem(s + d, nseq) for d in range(1, nseq)]
    joined = _greet([_at(h, p) for p in peers])
    tokens = pltpu.make_async_copy(x_hbm, x_ref, xsem)
    tokens.start()
    loads = []
    for j, w in enumerate((wq_ref, wk_ref, wv_ref)):
        for p in range(PARTS):
            c = pltpu.make_async_copy(
                w.at[pl.ds(p * rows, rows), pl.ds(first, cols)], wbuf.at[j, p], wsem.at[j, p])
            c.start()
            loads.append(c)
    ring = []
    for b in range(FIRST):
        for i, (src, dst) in enumerate(((k_hbm, kring), (v_hbm, vring))):
            pair = pl.ds(2 * b, 2)
            ring.append(pltpu.make_async_copy(src.at[pair], dst.at[pair], ringsem.at[i, b]))
    asked = 0
    sends = []
    tokens.wait()
    for j in range(3):
        acc = None
        for p in range(PARTS):
            loads[j * PARTS + p].wait()
            share = -(-len(ring) * (j * PARTS + p + 1) // (3 * PARTS))
            while asked < share:
                ring[asked].start()
                asked += 1
            part = jnp.dot(x_ref[:, p * rows:(p + 1) * rows], wbuf[j, p], preferred_element_type=F32)
            acc = part if acc is None else acc + part
        held[s, j] = acc.astype(BF16)
        if j == 0:
            joined()
        for i, p in enumerate(peers):
            c = pltpu.make_async_remote_copy(
                src_ref=held.at[s, j], dst_ref=held.at[s, j], send_sem=ssem.at[j, i], recv_sem=rsem.at[j, i],
                device_id=_at(h, p), device_id_type=MESH)
            c.start()
            sends.append(c)

    def spread(src, which):
        per = cols // 256
        for j in which:
            for i in range(per):
                for half in range(2):
                    val = held[src, j, :, i * 256 + half * 128:i * 256 + half * 128 + 128].astype(F32)
                    qkv_ref[j, half, pl.ds(src * per + i, val.shape[0], stride=nseq * per), :] = val

    spread(s, range(3))
    for j in range(3):
        for i in range(nseq - 1):
            sends[j * (nseq - 1) + i].wait_recv()
            spread(lax.rem(s + nseq - 1 - i, nseq), (j,))
    for c in sends:
        c.wait_send()
    for c in ring:
        c.wait()


def attend_kernel(scale, pos_ref, qkv_ref, k_hbm, v_hbm, kring_in, vring_in,
                  ko_hbm, vo_hbm, kring, vring, *rest):
    chunks = rest[:-9]
    kmore, vmore, obuf, mbuf, lbuf, kin, vin, kout, vout = rest[-9:]
    batch, wide, hd = k_hbm.shape
    nseq = len(chunks)
    heads = obuf.shape[1] // batch
    per = heads // nseq
    span = wide // heads
    pairs = batch // 2
    base = lax.axis_index("seq") * span
    col = lax.broadcasted_iota(jnp.int32, (heads, wide), 1)
    row = lax.broadcasted_iota(jnp.int32, (heads, wide), 0)
    own = lax.rem(col, heads) == row
    slot_of = jnp.where(own, base + col // heads, batch * nseq * span)

    def both(i):
        return pl.ds(i * 2, 2)

    def home(i):
        slot = SLOTS[i]
        return (kring, vring, slot, slot) if slot < RING else (kmore, vmore, slot - RING, slot)

    def reads(i):
        kbuf, vbuf, slot, sem = home(i)
        return [pltpu.make_async_copy(src.at[both(i)], dst.at[both(slot)], done.at[sem])
                for src, dst, done in ((k_hbm, kbuf, kin), (v_hbm, vbuf, vin))]

    def writes(i):
        kbuf, vbuf, slot, sem = home(i)
        return [pltpu.make_async_copy(src.at[both(slot)], dst.at[both(i)], done.at[sem])
                for src, dst, done in ((kbuf, ko_hbm, kout), (vbuf, vo_hbm, vout))]

    def fresh(j, lines):
        return jnp.concatenate([qkv_ref[j, 0, lines, :], qkv_ref[j, 1, lines, :]], axis=-1).astype(BF16)

    def begin(copies):
        for c in copies:
            c.start()

    def finish(copies):
        for c in copies:
            c.wait()

    def attend(i):
        kbuf, vbuf, slot, _ = home(i)
        rows = []
        for g in range(2):
            b = 2 * i + g
            pos = pos_ref[b]
            at = pos - base
            lines = pl.ds(b * heads, heads)
            spot = pl.ds(pl.multiple_of(at * heads, heads), heads)
            ks = 2 * slot + g

            @pl.when(jnp.logical_and(at >= 0, at < span))
            def _():
                kbuf[ks, spot, :] = fresh(1, lines)
                vbuf[ks, spot, :] = fresh(2, lines)

            rows.append((b, pos, lines, ks))
        scores = []
        for b, pos, lines, ks in rows:
            score = lax.dot_general(fresh(0, lines), kbuf[ks], NT, preferred_element_type=F32) * scale
            scores.append(jnp.where(slot_of <= pos, score, -jnp.inf))
        for (b, pos, lines, ks), score in zip(rows, scores):
            top = jnp.max(score, axis=-1, keepdims=True)
            safe = jnp.where(top == -jnp.inf, 0.0, top)
            weight = jnp.exp(score - safe)
            total = jnp.sum(weight, axis=-1, keepdims=True)
            mix = jnp.dot(weight.astype(BF16), vbuf[ks], preferred_element_type=F32)
            obuf[0, lines, :] = mix[:, :128]
            obuf[1, lines, :] = mix[:, 128:]
            mbuf[lines, :] = jnp.broadcast_to(top, (heads, 128))
            lbuf[lines, :] = jnp.broadcast_to(total, (heads, 128))

    for what, i in PLAN:
        if what == "r":
            begin(reads(i))
        elif what == "w":
            begin(writes(i))
        elif what == "R":
            finish(reads(i))
        elif what == "W":
            finish(writes(i))
        else:
            attend(i)
    eye = (lax.broadcasted_iota(jnp.int32, (batch, 128), 0)
           == lax.broadcasted_iota(jnp.int32, (batch, 128), 1))
    me = lax.axis_index("seq")
    for d, chunk in enumerate(chunks):
        for e in range(per):
            pick = pl.ds(_flip(me, d) * per + e, batch, stride=heads)
            rows = slice(e * batch, (e + 1) * batch)
            chunk[rows, :128] = obuf[0, pick, :]
            chunk[rows, 128:] = obuf[1, pick, :]
            for i, buf in enumerate((mbuf, lbuf)):
                line = per * batch + 2 * e + i
                chunk[line:line + 1, :128] = jnp.sum(jnp.where(eye, buf[pick, :], 0.0), axis=0, keepdims=True)
                chunk[line:line + 1, 128:] = jnp.zeros((1, hd - 128), F32)
        used = per * batch + 2 * per
        chunk[used:, :] = jnp.zeros((chunk.shape[0] - used, hd), F32)


def write_kernel(kring, vring, ko_in, vo_in, chunk, ko_hbm, vo_hbm, done, sem):
    pairs = ko_hbm.shape[0] // 2
    copies = []
    for i in range(pairs - KEPT, pairs):
        for src, dst in ((kring, ko_hbm), (vring, vo_hbm)):
            c = pltpu.make_async_copy(
                src.at[pl.ds(SLOTS[i] * 2, 2)], dst.at[pl.ds(i * 2, 2)], sem.at[len(copies)])
            c.start()
            copies.append(c)
    done[...] = jnp.zeros_like(done)
    for c in copies:
        c.wait()


def finish_kernel(*refs):
    got = refs[:-14]
    wo, after, y_ref, theirs, ours, half, ygot, yout, s1, r1, s2, r2, s3, r3 = refs[-14:]
    nseq = len(got)
    chips, batch, cols = ours.shape
    ndev = 2 * chips
    hd = got[0].shape[1]
    per = (got[0].shape[0] - 8) // batch
    h, s = lax.axis_index("head"), lax.axis_index("seq")
    me = h * nseq + s
    core, chip = lax.rem(me, 2), me // 2

    def spot(p):
        return _at(p // nseq, lax.rem(p, nseq))

    far = [_flip(me, d) for d in range(ndev - 1, 0, -1)]
    joined = _greet([spot(p) for p in far])
    eye = (lax.broadcasted_iota(jnp.int32, (batch, hd), 0)
           == lax.broadcasted_iota(jnp.int32, (batch, hd), 1))
    attn = []
    for e in range(per):
        line = per * batch + 2 * e
        tops = [got[i][line:line + 1, :] for i in range(nseq)]
        sums = [got[i][line + 1:line + 2, :] for i in range(nseq)]
        top = functools.reduce(jnp.maximum, tops)
        mix, total = None, None
        for i in range(nseq):
            factor = jnp.exp(tops[i] - top)
            share = factor * sums[i]
            total = share if total is None else total + share
            down = jnp.sum(jnp.where(eye, factor, 0.0), axis=1, keepdims=True)
            term = got[i][e * batch:(e + 1) * batch, :] * down
            mix = term if mix is None else mix + term
        down = jnp.sum(jnp.where(eye, total, 0.0), axis=1, keepdims=True)
        attn.append((mix / down).astype(BF16))
    attn = jnp.concatenate(attn, axis=-1)

    def product(j, side):
        at = pl.multiple_of((2 * j + side) * cols, 128)
        return jnp.dot(attn, wo[:, pl.ds(at, cols)], preferred_element_type=F32)

    route = [_flip(chip, d) for d in range(chips - 1, -1, -1)]
    for k, there in enumerate(route):
        theirs[k] = product(there, 1 - core)
    joined()
    swaps = []
    for k in range(chips):
        c = pltpu.make_async_remote_copy(
            src_ref=theirs.at[k], dst_ref=half.at[k], send_sem=s1.at[k], recv_sem=r1.at[k],
            device_id=spot(_flip(me, 1)), device_id_type=MESH)
        c.start()
        swaps.append(c)
    for k, there in enumerate(route):
        ours[k] = product(there, core)
    moves = []
    for k, there in enumerate(route):
        swaps[k].wait_recv()
        ours[k] += half[k]
        if k < chips - 1:
            c = pltpu.make_async_remote_copy(
                src_ref=ours.at[k], dst_ref=ygot.at[k], send_sem=s2.at[k], recv_sem=r2.at[k],
                device_id=spot(2 * there + core), device_id_type=MESH)
            c.start()
            moves.append(c)
    acc = ours[chips - 1]
    for i in range(chips - 2, -1, -1):
        moves[i].wait_recv()
        acc = acc + ygot[i]
    yout[me] = acc.astype(BF16)
    shares = []
    for i, p in enumerate(far):
        c = pltpu.make_async_remote_copy(
            src_ref=yout.at[me], dst_ref=yout.at[me], send_sem=s3.at[i], recv_sem=r3.at[i],
            device_id=spot(p), device_id_type=MESH)
        c.start()
        shares.append(c)
    for c in shares:
        c.wait_recv()
    for p in range(ndev):
        y_ref[:, p * cols:(p + 1) * cols] = yout[p]
    for c in swaps + moves + shares:
        c.wait_send()


def solution(mesh):
    nhead, nseq = mesh.shape["head"], mesh.shape["seq"]
    ndev = nhead * nseq
    cache_spec = P("rep", "seq", "head", None)
    any_spec = pl.BlockSpec(memory_space=pl.ANY)
    vmem = pl.BlockSpec(memory_space=pltpu.VMEM)
    smem = pl.BlockSpec(memory_space=pltpu.SMEM)

    def local_step(tokens, w_query, w_key, w_value, w_out, k_cache, v_cache, positions):
        batch, span, heads, hd = k_cache.shape
        model = tokens.shape[1]
        cols = heads * hd // nseq
        per = heads // nseq
        cache = jax.ShapeDtypeStruct((batch, span * heads, hd), BF16)
        ring = jax.ShapeDtypeStruct((2 * RING, span * heads, hd), BF16)
        k_flat, v_flat = k_cache.reshape(cache.shape), v_cache.reshape(cache.shape)
        dma = pltpu.SemaphoreType.DMA
        qkv, kring, vring = pl.pallas_call(
            project_kernel,
            out_shape=(jax.ShapeDtypeStruct((3, 2, batch * heads, 128), F32), ring, ring),
            in_specs=[any_spec] * 6,
            out_specs=(vmem, vmem, vmem),
            scratch_shapes=[
                pltpu.VMEM(tokens.shape, BF16),
                pltpu.VMEM((3, PARTS, model // PARTS, cols), BF16),
                pltpu.VMEM((nseq, 3, batch, cols), BF16),
                dma, dma((3, PARTS)), dma((2, FIRST)), dma((3, nseq - 1)), dma((3, nseq - 1)),
            ],
            compiler_params=pltpu.CompilerParams(
                collective_id=0, has_side_effects=True, vmem_limit_bytes=11 * 2**20),
        )(pltpu.with_memory_space_constraint(tokens, pltpu.HBM), w_query, w_key, w_value, k_flat, v_flat)
        chunk = jax.ShapeDtypeStruct((per * batch + 8, hd), F32)
        chunk = jax.ShapeDtypeStruct((per * batch + 8, hd), F32)
        k_out, v_out, kring, vring, *chunks = pl.pallas_call(
            functools.partial(attend_kernel, hd ** -0.5),
            out_shape=(cache, cache, ring, ring) + (chunk,) * nseq,
            in_specs=[smem, vmem, any_spec, any_spec, vmem, vmem],
            out_specs=(any_spec, any_spec, vmem, vmem) + (vmem,) * nseq,
            input_output_aliases={4: 2, 5: 3},
            scratch_shapes=[
                pltpu.VMEM((2 * MORE, span * heads, hd), BF16),
                pltpu.VMEM((2 * MORE, span * heads, hd), BF16),
                pltpu.VMEM((2, batch * heads, 128), F32),
                pltpu.VMEM((batch * heads, 128), F32),
                pltpu.VMEM((batch * heads, 128), F32),
                dma((RING + MORE,)), dma((RING + MORE,)), dma((RING + MORE,)), dma((RING + MORE,)),
            ],
            compiler_params=pltpu.CompilerParams(vmem_limit_bytes=11 * 2**20),
        )(positions, qkv, k_flat, v_flat, kring, vring)
        got = [lax.ppermute(chunks[d], "seq", [(i, i ^ d) for i in range(nseq)]) for d in range(1, nseq)]
        k_out, v_out, after = pl.pallas_call(
            write_kernel,
            out_shape=(cache, cache, jax.ShapeDtypeStruct((8, 128), F32)),
            in_specs=[vmem, vmem, any_spec, any_spec, vmem],
            out_specs=(any_spec, any_spec, vmem),
            input_output_aliases={2: 0, 3: 1},
            scratch_shapes=[dma((2 * KEPT,))],
            compiler_params=pltpu.CompilerParams(vmem_limit_bytes=1 * 2**20),
            cost_estimate=pl.CostEstimate(flops=10**9, bytes_accessed=2**24, transcendentals=0),
        )(kring, vring, k_out, v_out, chunks[0])
        ycols = model // ndev
        y = pl.pallas_call(
            finish_kernel,
            out_shape=jax.ShapeDtypeStruct((batch, model), BF16),
            in_specs=[vmem] * (nseq + 2),
            out_specs=vmem,
            scratch_shapes=[
                pltpu.VMEM((ndev // 2, batch, ycols), F32),
                pltpu.VMEM((ndev // 2, batch, ycols), F32),
                pltpu.VMEM((ndev // 2, batch, ycols), F32),
                pltpu.VMEM((ndev // 2 - 1, batch, ycols), F32),
                pltpu.VMEM((ndev, batch, ycols), BF16),
                dma((ndev // 2,)), dma((ndev // 2,)), dma((ndev // 2 - 1,)), dma((ndev // 2 - 1,)), dma((ndev - 1,)), dma((ndev - 1,)),
            ],
            compiler_params=pltpu.CompilerParams(
                collective_id=1, has_side_effects=True, vmem_limit_bytes=6 * 2**20),
        )(chunks[0], *got, w_out, after)
        return y, k_out.reshape(k_cache.shape), v_out.reshape(v_cache.shape)

    return jax.shard_map(
        local_step,
        mesh=mesh,
        in_specs=(P("rep", None), P(), P(), P(), P(("head", "seq"), None), cache_spec, cache_spec, P("rep")),
        out_specs=(P("rep", None), cache_spec, cache_spec),
        check_vma=False,
    )
```
